256 devices in a mesh: rep: 2 (over y), step: 32 (over z, core), patch: 4 (over x).
Axes of the slice: x: 4, y: 2, z: 16, core: 2. Of those that a mesh axis runs over, the one named last changes fastest.
The devices are a block of a 4x16x16 slice.
Arguments:
- latent_old: float32 [64, 1024, 64], P(('rep', 'step'), 'patch'), parts along dimension 0, may hold values from -6 to 6
- noise_start: float32 [2048, 64], P(('rep', 'patch')), parts along dimension 0, may hold values from -6 to 6
- step_index: int32 [64], P(('rep', 'step')), parts along dimension 0, may hold values from 0 to 998
- sigma_table: float32 [1000], replicated, may hold values from 0.02 to 1
- mod_weight: bfloat16 [256, 9216], replicated, may hold values from -0.375 to 0.375
- embed_weight: bfloat16 [64, 3072], replicated, may hold values from -0.75 to 0.75
- embed_bias: float32 [3072], replicated, may hold values from -3 to 3
- query_weight: bfloat16 [3072, 1536], P('step'), may hold values from -0.109375 to 0.109375
- query_gain: float32 [128], replicated, may hold values from 0.1 to 1.9
- stale_keys: bfloat16 [64, 1280, 1536], P(('rep', 'step'), 'patch'), parts along dimension 0, may hold values from -640 to 640
- stale_values: bfloat16 [64, 1280, 1536], P(('rep', 'step'), 'patch'), parts along dimension 0, may hold values from -6 to 6
- out_weight: bfloat16 [3072, 1536], P('step'), may hold values from -0.3125 to 0.3125
- final_weight: bfloat16 [3072, 64], replicated, may hold values from -0.109375 to 0.109375
Outputs:
- latent_new: float32 [64, 1024, 64], P(('rep', 'step'), 'patch'), parts along dimension 0
The draws below stay inside these ranges and needn't reach their ends.
There are 2 independent parts, one for each index of `rep`. The reference program is written for one: setup_inputs(seed, part) draws one part's arguments, and reference() takes and returns one part's arrays. A program takes and returns all parts, laid end to end along the dimension named above; an argument that names none is the same for every part. Nothing has to cross between parts.
All inputs are finite; a program needn't handle non-finite values.
Results may differ from the reference program's by a relative error of at most 0.012.
The reference program's roundings to bfloat16 on the way count: a program that leaves them out, or rounds other values in their place, can miss the bound.
Values may be sent and summed in bfloat16 or wider, within the bound.
No kernel may reach another device: no remote copies, remote signals or barrier semaphores. Data moves between devices by JAX's collectives and lax.ppermute only.
A program may use at most 128 MiB of HBM per device.

```python
import math
import jax
import jax.numpy as jnp
from jax import lax

D = 3072
HEAD = 128
C = 64
FREQ = 256
HEADS = 12
TABLE = 1000
STEPS = 32
TOKENS = 1024
KEYS = 1280


def draw_stale_keys(key, part):
    key_base = jax.random.fold_in(jax.random.fold_in(key, 11), 0)
    width = HEADS * HEAD
    base = 2.5 * jnp.clip(jax.random.normal(key_base, (STEPS, KEYS, width), jnp.float32), -6.0, 6.0)
    return base.astype(jnp.bfloat16)


def with_ends(entries, key, smallest, largest):
    spot = [jax.random.randint(jax.random.fold_in(key, axis), (), 0, length) for axis, length in enumerate(entries.shape)]
    longest = entries.shape.index(max(entries.shape))
    beside = spot[:longest] + [(spot[longest] + 1) % entries.shape[longest]] + spot[longest + 1:]
    return entries.at[tuple(spot)].set(smallest).at[tuple(beside)].set(largest)


def block_scale(rng, dims, cuts, least, largest):
    level = 1.0
    for axis_at, blocks in cuts:
        heights = jax.random.uniform(jax.random.fold_in(jax.random.fold_in(rng, 6), axis_at), (blocks,), jnp.float32, least / len(cuts), largest / len(cuts))
        level = level * jnp.repeat(jnp.exp(heights), dims[axis_at] // blocks).reshape((-1,) + (1,) * (len(dims) - 1 - axis_at))
    return level


def centred(rng, extent, scale, bound, pieces=(), kind=jnp.bfloat16):
    values = jax.random.normal(rng, extent, jnp.float32) * scale
    if len(pieces) > 0:
        values = block_scale(rng, extent, pieces, -0.22, 0.18) * values
    return jnp.clip(values, min=-bound, max=bound).astype(kind)


def setup_inputs(seed: int = 0, part: int = 0) -> dict:
    arg_keys = jax.random.split(jax.random.key(seed), 14)
    part_splits = jax.random.split(jax.random.fold_in(arg_keys[13], part), 14)
    latent_old = centred(part_splits[0], (STEPS, TOKENS, C), 1.0, 6.0, ((0, 32), (1, 4)), jnp.float32)
    noise_start = centred(part_splits[1], (TOKENS, C), 1.0, 6.0, ((0, 4),), jnp.float32)
    step_index = with_ends(jax.random.randint(part_splits[2], (STEPS,), 0, TABLE - 1), jax.random.fold_in(part_splits[2], 1), 0, (TABLE - 1) - 1).astype(jnp.int32)
    sigma_table = jnp.clip(jnp.exp(jax.random.uniform(arg_keys[3], (TABLE,), jnp.float32, math.log(0.02), math.log(1.0))), 0.02, 1.0)
    mod_weight = centred(arg_keys[4], (FREQ, 3 * D), FREQ ** -0.5, 0.375)
    embed_weight = centred(arg_keys[5], (C, D), C ** -0.5, 0.75)
    embed_bias = centred(arg_keys[6], (D,), 0.5, 3.0, (), jnp.float32)
    query_weight = centred(arg_keys[7], (D, HEADS * HEAD), D ** -0.5, 0.109375, ((0, 32),))
    query_gain = jnp.clip(1.0 + 0.18 * jax.random.normal(arg_keys[8], (HEAD,), jnp.float32), 0.1, 1.9)
    stale_keys = draw_stale_keys(jax.random.fold_in(jax.random.fold_in(arg_keys[13], part), 71), part)
    stale_values = centred(part_splits[10], (STEPS, KEYS, HEADS * HEAD), 1.0, 6.0, ((0, 32), (1, 4)))
    out_weight = centred(arg_keys[11], (D, HEADS * HEAD), (HEADS * HEAD // 4) ** -0.5, 0.3125, ((0, 32),))
    final_weight = centred(arg_keys[12], (D, C), D ** -0.5, 0.109375)
    return dict(latent_old=latent_old, noise_start=noise_start, step_index=step_index, sigma_table=sigma_table, mod_weight=mod_weight, embed_weight=embed_weight, embed_bias=embed_bias, query_weight=query_weight, query_gain=query_gain, stale_keys=stale_keys, stale_values=stale_values, out_weight=out_weight, final_weight=final_weight)


epsilon = 1e-06

def layer_norm(values_in):
    row_mean = lax.optimization_barrier(jnp.mean(values_in, axis=-1, keepdims=True))
    centered = values_in - row_mean
    row_var = lax.optimization_barrier(jnp.mean(centered * centered, axis=-1, keepdims=True))
    return centered * lax.rsqrt(row_var + epsilon)

def time_embed(sigma_now):
    half_count = FREQ // 2
    frequency = jnp.exp(-math.log(10000.0) * jnp.arange(half_count).astype(jnp.float32) / half_count)
    angles = 1000.0 * sigma_now * frequency
    return jnp.concatenate([jnp.cos(angles), jnp.sin(angles)])

def reference(latent_old, noise_start, step_index, sigma_table, mod_weight, embed_weight, embed_bias, query_weight, query_gain, stale_keys, stale_values, out_weight, final_weight):

    def one_step(items):
        latent, step_slot, keys_here, values_here = items
        sigma_now = sigma_table[step_slot]
        sigma_next = sigma_table[step_slot + 1]
        embedded = jax.nn.silu(time_embed(sigma_now)).astype(jnp.bfloat16)
        modulate = jnp.dot(embedded[None, :], mod_weight, preferred_element_type=jnp.float32)[0]
        shift_vec = modulate[:D]
        scale_vec = modulate[D:2 * D]
        gate_vec = modulate[2 * D:]
        hidden = jnp.dot(latent.astype(jnp.bfloat16), embed_weight, preferred_element_type=jnp.float32) + embed_bias
        normed = (layer_norm(hidden) * (1.0 + scale_vec) + shift_vec).astype(jnp.bfloat16)
        queries = jnp.dot(normed, query_weight, preferred_element_type=jnp.float32).reshape(TOKENS, HEADS, HEAD)
        queries = queries * lax.rsqrt(lax.optimization_barrier(jnp.mean(queries * queries, axis=-1, keepdims=True)) + epsilon) * query_gain
        queries = queries.astype(jnp.bfloat16).astype(jnp.float32)
        keys_split = keys_here.reshape(KEYS, HEADS, HEAD).astype(jnp.float32)
        values_split = values_here.reshape(KEYS, HEADS, HEAD).astype(jnp.float32)
        scores = jnp.einsum('qhd,khd->hqk', queries, keys_split) / math.sqrt(HEAD)
        row_peak = lax.optimization_barrier(jnp.max(scores, axis=-1, keepdims=True))
        exp_weights = jnp.exp(scores - row_peak)
        row_total = lax.optimization_barrier(jnp.sum(exp_weights, axis=-1))
        rounded = lax.optimization_barrier(exp_weights.astype(jnp.bfloat16)).astype(jnp.float32)
        blended = jnp.einsum('hqk,khd->hqd', rounded, values_split) / row_total[..., None]
        attended = jnp.transpose(blended, (1, 0, 2)).reshape(TOKENS, HEADS * HEAD).astype(jnp.bfloat16)
        branch = jnp.dot(attended, out_weight.T, preferred_element_type=jnp.float32)
        mixed = hidden + gate_vec * branch
        velocity = jnp.dot(layer_norm(mixed).astype(jnp.bfloat16), final_weight, preferred_element_type=jnp.float32)
        return velocity * (sigma_next - sigma_now)
    terms = lax.map(one_step, (latent_old, step_index, stale_keys, stale_values))
    return noise_start[None] + jnp.cumsum(terms, axis=0)
```

```python
import functools
import math

import jax
import jax.numpy as jnp
from jax import lax
from jax.experimental import pallas as pl
from jax.experimental.pallas import tpu as pltpu
from jax.sharding import Mesh
from jax.sharding import PartitionSpec as P

HEAD = 128
CORES = 2
STEP = ("chip", "core")
REP_STEP = ("rep", "chip", "core")
epsilon = 1e-06


def shift(value, axis, distance, wrap):
    size = lax.axis_size(axis)
    pairs = [(i, (i + distance) % size) for i in range(size) if wrap or 0 <= i + distance < size]
    return lax.ppermute(value, axis, pairs)


def ring_gather(shard, axis):
    size, here = lax.axis_size(axis), lax.axis_index(axis)
    held = jnp.zeros((size, *shard.shape), shard.dtype)

    def put(held, piece, owner):
        return lax.dynamic_update_slice_in_dim(held, piece[None], lax.rem(owner + size, size), 0)

    held = put(held, shard, here)
    up = down = shard
    for hop in range(1, size // 2 + 1):
        up = shift(up, axis, 1, True)
        held = put(held, up, here - hop)
        if hop < size - size // 2:
            down = shift(down, axis, -1, True)
            held = put(held, down, here + hop)
    return held


def both_cores(own, axis):
    other = shift(own, axis, 1, True)
    first = lax.axis_index(axis) == 0
    return jnp.stack([jnp.where(first, own, other), jnp.where(first, other, own)], axis=1)


def layer_norm(values_in):
    row_mean = jnp.mean(values_in, axis=-1, keepdims=True)
    centered = values_in - row_mean
    row_var = jnp.mean(centered * centered, axis=-1, keepdims=True)
    return centered * lax.rsqrt(row_var + epsilon)


def time_embed(sigma_now, half_count):
    frequency = jnp.exp(
        -math.log(10000.0) * jnp.arange(half_count).astype(jnp.float32) / half_count
    )
    angles = 1000.0 * sigma_now * frequency
    return jnp.concatenate([jnp.cos(angles), jnp.sin(angles)])


def attention_body(query_ref, gain_ref, key_ref, value_ref, out_ref):
    raw = query_ref[...]
    normed = raw * lax.rsqrt(jnp.mean(raw * raw, axis=-1, keepdims=True) + epsilon) * gain_ref[...]
    scores = lax.dot_general(
        normed.astype(jnp.bfloat16),
        key_ref[...],
        (((1,), (1,)), ((), ())),
        preferred_element_type=jnp.float32,
    )
    peak = jnp.max(scores, axis=-1, keepdims=True)
    weights = jnp.exp((scores - peak) * (1.0 / math.sqrt(HEAD)))
    total = jnp.sum(weights, axis=-1, keepdims=True)
    blended = jnp.dot(
        weights.astype(jnp.bfloat16), value_ref[...], preferred_element_type=jnp.float32
    )
    out_ref[...] = (blended / total).astype(jnp.bfloat16)


def attention(raw_queries, query_gain, keys, values):
    tokens, width = raw_queries.shape
    key_count = keys.shape[0]
    tile = min(256, tokens)
    heads = width // HEAD
    work = tokens * key_count * width
    return pl.pallas_call(
        attention_body,
        grid=(heads, tokens // tile),
        in_specs=[
            pl.BlockSpec((tile, HEAD), lambda h, t: (t, h)),
            pl.BlockSpec((1, HEAD), lambda h, t: (0, 0)),
            pl.BlockSpec((key_count, HEAD), lambda h, t: (0, h)),
            pl.BlockSpec((key_count, HEAD), lambda h, t: (0, h)),
        ],
        out_specs=pl.BlockSpec((tile, HEAD), lambda h, t: (t, h)),
        out_shape=jax.ShapeDtypeStruct((tokens, width), jnp.bfloat16),
        cost_estimate=pl.CostEstimate(
            flops=4 * work,
            bytes_accessed=4 * key_count * width + 6 * tokens * width,
            transcendentals=work // HEAD,
        ),
        name="attention",
    )(raw_queries, query_gain.reshape(1, HEAD), keys, values)


def prefix_over_steps(drift):
    core = lax.axis_index("core")
    rows = drift.shape[0] // CORES
    sent = drift.astype(jnp.bfloat16)
    other = shift(sent, "core", 1, True).astype(jnp.float32)
    within = jnp.where(core == 1, other, jnp.zeros_like(other))
    chip_total = drift + other
    mine = lax.dynamic_slice_in_dim(chip_total, core * rows, rows, 0)
    group = 4
    sent = mine.astype(jnp.bfloat16)
    near = [shift(sent, "chip", d, False) for d in range(1, group)]
    before = functools.reduce(lambda a, b: a + b, [n.astype(jnp.float32) for n in near])
    window = (mine + before).astype(jnp.bfloat16)
    size = lax.axis_size("chip")
    far = [shift(window, "chip", d, False) for d in range(group, size, group)]
    before = functools.reduce(lambda a, b: a + b, [f.astype(jnp.float32) for f in far], before)
    halves = lax.all_gather(before.astype(jnp.bfloat16), "core", axis=0, tiled=True)
    return within + halves.astype(jnp.float32)


def per_device(
    latent_old,
    noise_start,
    step_index,
    sigma_table,
    mod_weight,
    embed_weight,
    embed_bias,
    query_weight,
    query_gain,
    stale_keys,
    stale_values,
    out_weight,
    final_weight,
):
    parts, part = lax.axis_size("patch"), lax.axis_index("patch")
    width = embed_weight.shape[1]
    columns = query_weight.shape[1] // parts
    latent = latent_old[0].astype(jnp.bfloat16)
    token_count, channels = latent.shape
    key_rows = stale_keys.shape[1]

    all_out_weight = lax.all_gather(out_weight, STEP, axis=0, tiled=True)

    def by_part(rows):
        return jnp.moveaxis(rows.reshape(rows.shape[0], parts, columns), 1, 0)

    spare = -(-latent.size // columns)
    spare += -spare % 16
    packed = jnp.pad(latent.reshape(-1), (0, spare * columns - latent.size))
    packed = jnp.broadcast_to(packed.reshape(1, spare, columns), (parts, spare, columns))
    sent = [by_part(stale_keys[0]), by_part(stale_values[0]), packed]
    got = lax.all_to_all(jnp.concatenate(sent, axis=1), "patch", 0, 0, tiled=True)
    keys = got[:, :key_rows].reshape(-1, columns)
    values = got[:, key_rows : 2 * key_rows].reshape(-1, columns)
    all_latent = got[:, 2 * key_rows :].reshape(parts, -1)[:, : latent.size]
    all_latent = all_latent.reshape(parts * token_count, channels)

    my_columns = lax.dynamic_slice_in_dim(query_weight, part * columns, columns, 1)
    gathered = both_cores(ring_gather(my_columns, "chip"), "core").reshape(-1, columns)

    step_slot = step_index[0]
    table_slots = jnp.arange(sigma_table.shape[0])
    sigma_now = jnp.sum(jnp.where(table_slots == step_slot, sigma_table, 0.0))
    sigma_next = jnp.sum(jnp.where(table_slots == step_slot + 1, sigma_table, 0.0))
    embedded = jax.nn.silu(time_embed(sigma_now, mod_weight.shape[0] // 2)).astype(jnp.bfloat16)
    modulate = jnp.dot(embedded[None, :], mod_weight, preferred_element_type=jnp.float32)[0]
    shift_vec = modulate[:width]
    scale_vec = modulate[width : 2 * width]
    gate_vec = modulate[2 * width :]

    def embed(rows):
        return jnp.dot(rows, embed_weight, preferred_element_type=jnp.float32) + embed_bias

    normed = (layer_norm(embed(all_latent)) * (1.0 + scale_vec) + shift_vec).astype(jnp.bfloat16)
    normed = lax.optimization_barrier(normed)
    raw_queries = jnp.dot(normed, gathered, preferred_element_type=jnp.float32)
    attended = attention(raw_queries, query_gain, keys, values)
    attended = lax.all_to_all(
        attended.reshape(parts, token_count, columns), "patch", 0, 0, tiled=True
    )
    attended = jnp.moveaxis(attended, 0, 1).reshape(token_count, -1)
    hidden = embed(latent)
    branch = lax.dot_general(
        attended, all_out_weight, (((1,), (1,)), ((), ())), preferred_element_type=jnp.float32
    )
    mixed = hidden + gate_vec * branch
    velocity = jnp.dot(
        layer_norm(mixed).astype(jnp.bfloat16), final_weight, preferred_element_type=jnp.float32
    )
    drift_term = (velocity * (sigma_next - sigma_now)).reshape(-1, HEAD)
    prefix = prefix_over_steps(drift_term)
    return (noise_start + (prefix + drift_term).reshape(token_count, -1))[None]


def solution(mesh):
    shape = mesh.shape
    torus = Mesh(
        mesh.devices.reshape(shape["rep"], shape["step"] // CORES, CORES, shape["patch"]),
        ("rep", "chip", "core", "patch"),
    )
    placed = (
        P(REP_STEP, "patch", None),
        P(("rep", "patch"), None),
        P(REP_STEP),
        P(),
        P(),
        P(),
        P(),
        P(STEP, None),
        P(),
        P(REP_STEP, "patch", None),
        P(REP_STEP, "patch", None),
        P(STEP, None),
        P(),
    )
    return jax.shard_map(
        per_device,
        mesh=torus,
        in_specs=placed,
        out_specs=P(REP_STEP, "patch", None),
        check_vma=False,
    )
```

```python
import functools
import math

import jax
import jax.numpy as jnp
from jax import lax
from jax.experimental import pallas as pl
from jax.experimental.pallas import tpu as pltpu
from jax.sharding import Mesh
from jax.sharding import PartitionSpec as P

HEAD = 128
CORES = 2
EXTRA = 16
STEP = ("chip", "core")
REP_STEP = ("rep", "chip", "core")
epsilon = 1e-06


def shift(value, axis, distance, wrap):
    size = lax.axis_size(axis)
    pairs = [(i, (i + distance) % size) for i in range(size) if wrap or 0 <= i + distance < size]
    return lax.ppermute(value, axis, pairs)


def swap_cores(value):
    return lax.ppermute(value, "core", [(0, 1), (1, 0)])


def send_by_core(value, first, second, wrap):
    chips = lax.axis_size("chip")
    pairs = []
    for core, distance in enumerate((first, second)):
        for chip in range(chips):
            target = chip + (distance or 0)
            if distance is not None and (wrap or 0 <= target < chips):
                pairs.append((chip * CORES + core, target % chips * CORES + core))
    return lax.ppermute(value, ("chip", "core"), pairs)


def gather_rows(shard, tasks):
    chips, here, core = lax.axis_size("chip"), lax.axis_index("chip"), lax.axis_index("core")
    other = swap_cores(shard)
    piece = jnp.concatenate([jnp.where(core == 0, shard, other), jnp.where(core == 0, other, shard)])
    rows = piece.shape[0]
    step = jnp.where(core == 0, 1, -1)
    half = chips // 2
    pieces, waiting, results = [(0, piece)], [], {}
    for hop in range(1, half + 1):
        sent = send_by_core(piece, 1, -1, True)
        if hop in tasks:
            task, inputs = tasks[hop]
            if callable(inputs):
                inputs = inputs(results)
            _, inputs = lax.optimization_barrier((piece, inputs))
            results[hop] = task(*inputs)
            sent, results[hop] = lax.optimization_barrier((sent, results[hop]))
        piece = sent
        pieces.append((hop, piece))
        if 2 * hop != chips:
            waiting.append((hop, piece))
        if hop in (half // 2, half - 1):
            swapped = swap_cores(jnp.concatenate([p for _, p in waiting]))
            for i, (at, _) in enumerate(waiting):
                pieces.append((-at, swapped[i * rows : (i + 1) * rows]))
            waiting = []
    held = jnp.zeros((chips, *piece.shape), shard.dtype)
    for at, piece in pieces:
        owner = lax.rem(here - at * step + chips, chips)
        held = lax.dynamic_update_slice_in_dim(held, piece[None], owner, 0)
    return held, results


def time_embed(sigma_now, half_count):
    frequency = jnp.exp(
        -math.log(10000.0) * jnp.arange(half_count).astype(jnp.float32) / half_count
    )
    angles = 1000.0 * sigma_now * frequency
    return jnp.concatenate([jnp.cos(angles), jnp.sin(angles)])


def pack_body(key_ref, value_ref, latent_ref, spread_ref, out_ref):
    rows = key_ref.shape[0]
    channels, tokens = latent_ref.shape
    out_ref[0, :rows] = key_ref[...]
    out_ref[0, rows : 2 * rows] = value_ref[...]
    spread = spread_ref[...]
    coarse = spread.astype(jnp.bfloat16).astype(jnp.float32)
    tail = jnp.concatenate(
        [
            latent_ref[...],
            jnp.ones_like(spread),
            coarse,
            spread - coarse,
            jnp.zeros((EXTRA - 3, tokens), jnp.float32),
        ]
    )
    out_ref[0, 2 * rows :] = jnp.zeros((channels + EXTRA, out_ref.shape[2]), jnp.bfloat16)
    out_ref[0, 2 * rows :, :tokens] = tail.astype(jnp.bfloat16)


def pack(keys, values, latent, spread, parts):
    rows, width = keys.shape
    channels, tokens = latent.shape
    columns = width // parts
    height = 2 * rows + channels + EXTRA
    return pl.pallas_call(
        pack_body,
        grid=(parts,),
        in_specs=[
            pl.BlockSpec((rows, columns), lambda p: (0, p)),
            pl.BlockSpec((rows, columns), lambda p: (0, p)),
            pl.BlockSpec((channels, tokens), lambda p: (0, 0)),
            pl.BlockSpec((1, tokens), lambda p: (0, 0)),
        ],
        out_specs=pl.BlockSpec((1, height, columns), lambda p: (p, 0, 0)),
        out_shape=jax.ShapeDtypeStruct((parts, height, columns), jnp.bfloat16),
        cost_estimate=pl.CostEstimate(
            flops=parts * height * columns,
            bytes_accessed=4 * parts * height * columns,
            transcendentals=0,
        ),
        name="pack",
    )(keys, values, latent, spread)


def attention_body(parts, rows, packed_ref, project_ref, gain_ref, out_ref, even_ref, odd_ref):
    at, last = pl.program_id(0), pl.num_programs(0) - 2
    now, past = jnp.minimum(at, last), jnp.maximum(at - 1, 0)
    tile = even_ref.shape[0]
    head, part = now // parts, lax.rem(now, parts)

    def columns(head):
        return pl.ds(pl.multiple_of(head * HEAD, HEAD), HEAD)

    def run(now_ref, past_ref):
        tokens = packed_ref[part, 2 * rows :, :tile]
        both = lax.dot_general(
            jnp.concatenate([tokens, tokens]),
            project_ref[head],
            (((0,), (0,)), ((), ())),
            preferred_element_type=jnp.float32,
        )
        raw, spread = both[:, :HEAD], both[:, HEAD:]
        square = jnp.mean(raw * raw, axis=-1, keepdims=True) + epsilon * (spread * spread)
        queries = (raw * lax.rsqrt(square) * gain_ref[...]).astype(jnp.bfloat16)
        for p in range(parts):
            now_ref[:, p * rows : (p + 1) * rows] = lax.dot_general(
                queries,
                packed_ref[p, :rows, columns(head)],
                (((1,), (1,)), ((), ())),
                preferred_element_type=jnp.float32,
            )
        peak = jnp.max(past_ref[...], axis=-1, keepdims=True)
        weights = jnp.exp((past_ref[...] - peak) * (1.0 / math.sqrt(HEAD)))
        total = jnp.sum(weights, axis=-1, keepdims=True)
        values = packed_ref[:, rows : 2 * rows, columns(past // parts)].reshape(-1, HEAD)
        blended = jnp.dot(weights.astype(jnp.bfloat16), values, preferred_element_type=jnp.float32)
        out_ref[...] = (blended / total).astype(jnp.bfloat16)

    @pl.when(lax.rem(at, 2) == 0)
    def _():
        run(even_ref, odd_ref)

    @pl.when(lax.rem(at, 2) == 1)
    def _():
        run(odd_ref, even_ref)


def attention(project, query_gain, packed, rows, tile):
    parts, height, width = packed.shape
    tokens = parts * tile
    heads = width // HEAD
    work = tokens * parts * rows * width

    def past(i):
        at = jnp.maximum(i - 1, 0)
        return lax.rem(at, parts), at // parts

    whole = pl.BlockSpec(memory_space=pltpu.VMEM)
    return pl.pallas_call(
        functools.partial(attention_body, parts, rows),
        grid=(heads * parts + 1,),
        in_specs=[whole, whole, whole],
        out_specs=pl.BlockSpec((tile, HEAD), past),
        out_shape=jax.ShapeDtypeStruct((tokens, width), jnp.bfloat16),
        scratch_shapes=[pltpu.VMEM((tile, parts * rows), jnp.float32)] * 2,
        cost_estimate=pl.CostEstimate(
            flops=4 * work,
            bytes_accessed=4 * parts * rows * width + 6 * tokens * width,
            transcendentals=work // HEAD,
        ),
        name="attention",
    )(packed, project, query_gain.reshape(1, HEAD))


def finish_body(
    tile, attended_ref, weight_ref, hidden_ref, gate_ref, final_ref, out_ref, joined_ref, mixed_ref, sum_ref
):
    at = pl.program_id(0)
    parts, tokens, columns = attended_ref.shape

    @pl.when(at == 0)
    def _():
        for p in range(parts):
            joined_ref[:, p * columns : (p + 1) * columns] = attended_ref[p]
        sum_ref[...] = jnp.zeros_like(sum_ref)

    branch = lax.dot_general(
        joined_ref[...], weight_ref[...], (((1,), (1,)), ((), ())), preferred_element_type=jnp.float32
    )
    mixed = hidden_ref[:, pl.ds(pl.multiple_of(at * tile, tile), tile)] + gate_ref[...] * branch
    mixed_ref[at] = mixed
    sum_ref[...] += jnp.sum(mixed, axis=-1, keepdims=True)

    @pl.when(at == pl.num_programs(0) - 1)
    def _():
        count = mixed_ref.shape[0]
        width = count * tile
        mean = sum_ref[...] / width
        squares = functools.reduce(
            lambda a, b: a + b, [jnp.square(mixed_ref[i] - mean) for i in range(count)]
        )
        scale = lax.rsqrt(jnp.sum(squares, axis=-1, keepdims=True) / width + epsilon)
        out_ref[...] = functools.reduce(
            lambda a, b: a + b,
            [
                lax.dot_general(
                    final_ref[:, i * tile : (i + 1) * tile],
                    ((mixed_ref[i] - mean) * scale).astype(jnp.bfloat16),
                    (((1,), (1,)), ((), ())),
                    preferred_element_type=jnp.float32,
                )
                for i in range(count)
            ],
        )


def finish(attended, out_weight, hidden, gate, final_weight):
    parts, tokens, columns = attended.shape
    width, depth = out_weight.shape
    channels = final_weight.shape[1]
    tile = min(512, width)
    return pl.pallas_call(
        functools.partial(finish_body, tile),
        grid=(width // tile,),
        in_specs=[
            pl.BlockSpec(memory_space=pltpu.VMEM),
            pl.BlockSpec((tile, depth), lambda i: (i, 0)),
            pl.BlockSpec(memory_space=pltpu.VMEM),
            pl.BlockSpec((1, tile), lambda i: (0, i)),
            pl.BlockSpec((channels, width), lambda i: (0, 0)),
        ],
        out_specs=pl.BlockSpec((channels, tokens), lambda i: (0, 0)),
        out_shape=jax.ShapeDtypeStruct((channels, tokens), jnp.float32),
        scratch_shapes=[
            pltpu.VMEM((tokens, depth), jnp.bfloat16),
            pltpu.VMEM((width // tile, tokens, tile), jnp.float32),
            pltpu.VMEM((tokens, 1), jnp.float32),
        ],
        cost_estimate=pl.CostEstimate(
            flops=2 * tokens * width * (depth + channels),
            bytes_accessed=2 * width * depth + 4 * tokens * width,
            transcendentals=0,
        ),
        name="finish",
    )(attended, out_weight, hidden, gate.reshape(1, width), final_weight.T)


def prefix_over_steps(drift):
    half = jnp.bfloat16

    def wide(value):
        return value.astype(jnp.float32)

    other = wide(swap_cores(drift.astype(half)))
    within = jnp.where(lax.axis_index("core") == 1, other, jnp.zeros_like(other))
    here = drift + other
    near = wide(shift(here.astype(half), "chip", 1, False))
    near = near + wide(shift((here + near).astype(half), "chip", 2, False))
    window = (here + near).astype(half)
    chips = lax.axis_size("chip")
    far = send_by_core(window, 4, chips - 4, False)
    far = wide(far) + wide(send_by_core(far, 4, None, False))
    return within + near + far + wide(swap_cores(far.astype(half)))


def per_device(
    latent_old,
    noise_start,
    step_index,
    sigma_table,
    mod_weight,
    embed_weight,
    embed_bias,
    query_weight,
    query_gain,
    stale_keys,
    stale_values,
    out_weight,
    final_weight,
):
    parts, part = lax.axis_size("patch"), lax.axis_index("patch")
    width = embed_weight.shape[1]
    columns = query_weight.shape[1] // parts
    latent = latent_old[0].T
    channels, token_count = latent.shape
    key_rows = stale_keys.shape[1]

    all_out_weight = lax.all_gather(out_weight, STEP, axis=0, tiled=True)

    def embed(latent, embed_weight, embed_bias):
        hidden = lax.dot_general(
            latent.astype(jnp.bfloat16),
            embed_weight,
            (((0,), (0,)), ((), ())),
            preferred_element_type=jnp.float32,
        )
        hidden = hidden + embed_bias
        row_mean = jnp.mean(hidden, axis=-1, keepdims=True)
        row_var = jnp.mean(jnp.square(hidden - row_mean), axis=-1)
        return hidden, jnp.sqrt(row_var + epsilon)[None]

    def modulation(step_index, sigma_table, mod_weight):
        slots = jnp.arange(sigma_table.shape[0])
        sigma_now = jnp.sum(jnp.where(slots == step_index[0], sigma_table, 0.0))
        sigma_next = jnp.sum(jnp.where(slots == step_index[0] + 1, sigma_table, 0.0))
        embedded = jax.nn.silu(time_embed(sigma_now, mod_weight.shape[0] // 2)).astype(jnp.bfloat16)
        modulate = jnp.dot(embedded[None, :], mod_weight, preferred_element_type=jnp.float32)[0]
        return modulate, sigma_next - sigma_now

    def split(value):
        coarse = value.astype(jnp.bfloat16)
        return jnp.concatenate([coarse, (value - coarse.astype(jnp.float32)).astype(jnp.bfloat16)])

    def sources(modulate, embed_weight, embed_bias):
        shift_vec, scale_vec = modulate[:width], modulate[width : 2 * width]
        weight = embed_weight.astype(jnp.float32)
        centered = jnp.concatenate(
            [
                weight - jnp.mean(weight, axis=-1, keepdims=True),
                (embed_bias - jnp.mean(embed_bias))[None],
            ]
        )
        rows = [
            centered * (1.0 + scale_vec),
            shift_vec[None],
            shift_vec[None],
            jnp.zeros((EXTRA - 3, width), jnp.float32),
        ]
        return split(jnp.concatenate(rows))

    my_columns = lax.dynamic_slice_in_dim(query_weight, part * columns, columns, 1)
    tasks = {
        1: (embed, (latent, embed_weight, embed_bias)),
        2: (
            functools.partial(pack, parts=parts),
            lambda done: (stale_keys[0], stale_values[0], latent, done[1][1]),
        ),
        4: (modulation, (step_index, sigma_table, mod_weight)),
        6: (sources, lambda done: (done[4][0], embed_weight, embed_bias)),
    }
    gathered, done = gather_rows(my_columns, tasks)
    hidden, (modulate, delta), source = done[1][0], done[4], done[6]
    packed = lax.all_to_all(done[2], "patch", 0, 0, tiled=True)

    project = jnp.dot(source, gathered.reshape(width, columns), preferred_element_type=jnp.float32)
    deep = channels + EXTRA
    project = split(project[:deep] + project[deep:])
    project = jnp.moveaxis(project.reshape(2 * deep, -1, HEAD), 1, 0)
    row = lax.broadcasted_iota(jnp.int32, (1, 2 * deep, HEAD), 1)
    picks = jnp.where((row == channels + 1) | (row == channels + 2), 1.0, 0.0).astype(jnp.bfloat16)
    project = jnp.concatenate([project, jnp.broadcast_to(picks, project.shape)], axis=2)

    attended = attention(project, query_gain, packed, key_rows, token_count)
    attended = lax.all_to_all(
        attended.reshape(parts, token_count, columns), "patch", 0, 0, tiled=True
    )
    velocity = finish(attended, all_out_weight, hidden, modulate[2 * width :], final_weight)
    drift = velocity * delta
    return (noise_start.T + (prefix_over_steps(drift) + drift)).T[None]


def solution(mesh):
    shape = mesh.shape
    torus = Mesh(
        mesh.devices.reshape(shape["rep"], shape["step"] // CORES, CORES, shape["patch"]),
        ("rep", "chip", "core", "patch"),
    )
    placed = (
        P(REP_STEP, "patch", None),
        P(("rep", "patch"), None),
        P(REP_STEP),
        P(),
        P(),
        P(),
        P(),
        P(STEP, None),
        P(),
        P(REP_STEP, "patch", None),
        P(REP_STEP, "patch", None),
        P(STEP, None),
        P(),
    )
    return jax.shard_map(
        per_device,
        mesh=torus,
        in_specs=placed,
        out_specs=P(REP_STEP, "patch", None),
        check_vma=False,
    )
```

```python
import functools
import math

import jax
import jax.numpy as jnp
from jax import lax
from jax.experimental import pallas as pl
from jax.experimental.pallas import tpu as pltpu
from jax.sharding import Mesh
from jax.sharding import PartitionSpec as P

HEAD = 128
CORES = 2
EXTRA = 16
PAIR = 2
STEP = ("chip", "core")
REP_STEP = ("rep", "chip", "core")
epsilon = 1e-06


def shift(value, axis, distance, wrap):
    size = lax.axis_size(axis)
    pairs = [(i, (i + distance) % size) for i in range(size) if wrap or 0 <= i + distance < size]
    return lax.ppermute(value, axis, pairs)


def swap_cores(value):
    return lax.ppermute(value, "core", [(0, 1), (1, 0)])


def send_by_core(value, first, second, wrap):
    chips = lax.axis_size("chip")
    pairs = []
    for core, distance in enumerate((first, second)):
        for chip in range(chips):
            target = chip + (distance or 0)
            if distance is not None and (wrap or 0 <= target < chips):
                pairs.append((chip * CORES + core, target % chips * CORES + core))
    return lax.ppermute(value, ("chip", "core"), pairs)


def gather_rows(piece, tasks):
    chips, here = lax.axis_size("chip"), lax.axis_index("chip")
    step = jnp.where(lax.axis_index("core") == 0, 1, -1)
    half = chips // 2
    held = [jnp.zeros((chips, *p.shape), p.dtype) for p in piece]

    def put(held, piece, at):
        owner = lax.rem(here - at * step + chips, chips)
        return [lax.dynamic_update_slice_in_dim(h, p[None], owner, 0) for h, p in zip(held, piece)]

    held = put(held, piece, 0)
    waiting, results = [], {}
    for hop in range(1, half + 1):
        sent = tuple(send_by_core(p, 1, -1, True) for p in piece)
        if hop in tasks:
            task, inputs = tasks[hop]
            if callable(inputs):
                inputs = inputs(results)
            _, inputs = lax.optimization_barrier((piece, inputs))
            results[hop] = task(*inputs)
            sent, results[hop] = lax.optimization_barrier((sent, results[hop]))
        piece = sent
        held = put(held, piece, hop)
        if 2 * hop != chips:
            waiting.append((hop, piece))
        if hop in (half // 2, half - 1):
            for i in range(len(piece)):
                swapped = swap_cores(jnp.concatenate([p[i] for _, p in waiting]))
                for j, (at, p) in enumerate(waiting):
                    rows = p[i].shape[0]
                    held[i] = put([held[i]], [swapped[j * rows : (j + 1) * rows]], -at)[0]
            waiting = []
    return held, results


def time_embed(sigma_now, half_count):
    frequency = jnp.exp(
        -math.log(10000.0) * jnp.arange(half_count).astype(jnp.float32) / half_count
    )
    angles = 1000.0 * sigma_now * frequency
    return jnp.concatenate([jnp.cos(angles), jnp.sin(angles)])


def pack_body(key_ref, value_ref, latent_ref, spread_ref, out_ref):
    rows = key_ref.shape[0]
    channels, tokens = latent_ref.shape
    out_ref[0, :rows] = key_ref[...]
    out_ref[0, rows : 2 * rows] = value_ref[...]
    spread = spread_ref[...]
    coarse = spread.astype(jnp.bfloat16).astype(jnp.float32)
    tail = jnp.concatenate(
        [
            latent_ref[...],
            jnp.ones_like(spread),
            coarse,
            spread - coarse,
            jnp.zeros((EXTRA - 3, tokens), jnp.float32),
        ]
    )
    out_ref[0, 2 * rows :] = jnp.zeros((channels + EXTRA, out_ref.shape[2]), jnp.bfloat16)
    out_ref[0, 2 * rows :, :tokens] = tail.astype(jnp.bfloat16)


def pack(keys, values, latent, spread, parts):
    rows, width = keys.shape
    channels, tokens = latent.shape
    columns = width // parts
    height = 2 * rows + channels + EXTRA
    return pl.pallas_call(
        pack_body,
        grid=(parts,),
        in_specs=[
            pl.BlockSpec((rows, columns), lambda p: (0, p)),
            pl.BlockSpec((rows, columns), lambda p: (0, p)),
            pl.BlockSpec((channels, tokens), lambda p: (0, 0)),
            pl.BlockSpec((1, tokens), lambda p: (0, 0)),
        ],
        out_specs=pl.BlockSpec((1, height, columns), lambda p: (p, 0, 0)),
        out_shape=jax.ShapeDtypeStruct((parts, height, columns), jnp.bfloat16),
        cost_estimate=pl.CostEstimate(
            flops=parts * height * columns,
            bytes_accessed=4 * parts * height * columns,
            transcendentals=0,
        ),
        name="pack",
    )(keys, values, latent, spread)


def attention_body(parts, rows, packed_ref, project_ref, gain_ref, out_ref, even_ref, odd_ref):
    at, last = pl.program_id(0), pl.num_programs(0) - 2
    now, past = jnp.minimum(at, last), jnp.maximum(at - 1, 0)
    tile = even_ref.shape[0]
    head, part = now // parts, lax.rem(now, parts)

    def columns(head):
        return pl.ds(pl.multiple_of(head * HEAD, HEAD), HEAD)

    def run(now_ref, past_ref):
        tokens = packed_ref[part, 2 * rows :, :tile]
        both = lax.dot_general(
            jnp.concatenate([tokens, tokens]),
            project_ref[head],
            (((0,), (0,)), ((), ())),
            preferred_element_type=jnp.float32,
        )
        raw, spread = both[:, :HEAD], both[:, HEAD:]
        square = jnp.mean(raw * raw, axis=-1, keepdims=True) + epsilon * (spread * spread)
        queries = (raw * lax.rsqrt(square) * gain_ref[...]).astype(jnp.bfloat16)
        for p in range(parts):
            now_ref[:, p * rows : (p + 1) * rows] = lax.dot_general(
                queries,
                packed_ref[p, :rows, columns(head)],
                (((1,), (1,)), ((), ())),
                preferred_element_type=jnp.float32,
            )
        peak = jnp.max(past_ref[...], axis=-1, keepdims=True)
        weights = jnp.exp((past_ref[...] - peak) * (1.0 / math.sqrt(HEAD)))
        total = jnp.sum(weights, axis=-1, keepdims=True)
        values = packed_ref[:, rows : 2 * rows, columns(past // parts)].reshape(-1, HEAD)
        blended = jnp.dot(weights.astype(jnp.bfloat16), values, preferred_element_type=jnp.float32)
        out_ref[...] = jnp.broadcast_to((blended / total).astype(jnp.bfloat16), out_ref.shape)

    @pl.when(lax.rem(at, 2) == 0)
    def _():
        run(even_ref, odd_ref)

    @pl.when(lax.rem(at, 2) == 1)
    def _():
        run(odd_ref, even_ref)


def attention(project, query_gain, packed, rows, tile):
    parts, height, width = packed.shape
    tokens = parts * tile
    heads = width // HEAD
    work = tokens * parts * rows * width

    def past(i):
        at = jnp.maximum(i - 1, 0)
        part = lax.rem(at, parts)
        return part // PAIR, lax.rem(part, PAIR), at // parts

    whole = pl.BlockSpec(memory_space=pltpu.VMEM)
    return pl.pallas_call(
        functools.partial(attention_body, parts, rows),
        grid=(heads * parts + 1,),
        in_specs=[whole, whole, whole],
        out_specs=pl.BlockSpec((PAIR, tile, HEAD), past),
        out_shape=jax.ShapeDtypeStruct((parts, PAIR * tile, width), jnp.bfloat16),
        scratch_shapes=[pltpu.VMEM((tile, parts * rows), jnp.float32)] * 2,
        cost_estimate=pl.CostEstimate(
            flops=4 * work,
            bytes_accessed=4 * parts * rows * width + 6 * tokens * width,
            transcendentals=work // HEAD,
        ),
        name="attention",
    )(packed, project, query_gain.reshape(1, HEAD))


def finish_body(
    tile,
    attended_ref,
    weight_ref,
    latent_ref,
    embed_ref,
    bias_ref,
    gate_ref,
    final_ref,
    out_ref,
    joined_ref,
    mixed_ref,
    sum_ref,
):
    at = pl.program_id(0)
    parts, tokens, columns = attended_ref.shape
    channels = latent_ref.shape[1]

    @pl.when(at == 0)
    def _():
        for p in range(parts):
            joined_ref[:, p * columns : (p + 1) * columns] = attended_ref[p]
        sum_ref[...] = jnp.zeros_like(sum_ref)

    branch = lax.dot_general(
        joined_ref[...], weight_ref[...], (((1,), (1,)), ((), ())), preferred_element_type=jnp.float32
    )
    latent = jnp.concatenate([latent_ref[i] for i in range(PAIR)], axis=1)
    hidden = lax.dot_general(
        latent, embed_ref[...], (((0,), (1,)), ((), ())), preferred_element_type=jnp.float32
    )
    mixed = hidden + bias_ref[...] + gate_ref[...] * branch
    mixed_ref[at] = mixed
    sum_ref[...] += jnp.sum(mixed, axis=-1, keepdims=True)

    @pl.when(at == pl.num_programs(0) - 1)
    def _():
        count = mixed_ref.shape[0]
        mean = sum_ref[...] / (count * tile)
        squares = jnp.zeros_like(mean)
        product = jnp.zeros((channels, tokens), jnp.float32)
        for i in range(count):
            centered = mixed_ref[i] - mean
            squares += jnp.sum(centered * centered, axis=-1, keepdims=True)
            product += lax.dot_general(
                final_ref[i * tile : (i + 1) * tile],
                centered.astype(jnp.bfloat16),
                (((0,), (1,)), ((), ())),
                preferred_element_type=jnp.float32,
            )
        lane = lax.broadcasted_iota(jnp.int32, (tokens, HEAD), 1)
        sums = jnp.where(lane == 0, mean, jnp.where(lane == 1, squares, 0.0)).T[:8]
        whole = jnp.concatenate([product, sums])
        for i in range(PAIR):
            out_ref[i] = whole[:, i * (tokens // PAIR) : (i + 1) * (tokens // PAIR)]


def finish(attended, out_weight, latent, embed_rows, embed_bias, gate, final_weight):
    parts, tokens, columns = attended.shape
    width, depth = out_weight.shape
    channels = latent.shape[1]
    tile = min(512, width)
    whole = pl.BlockSpec(memory_space=pltpu.VMEM)
    return pl.pallas_call(
        functools.partial(finish_body, tile),
        grid=(width // tile,),
        in_specs=[
            whole,
            pl.BlockSpec((tile, depth), lambda i: (i, 0)),
            whole,
            pl.BlockSpec((tile, channels), lambda i: (i, 0)),
            pl.BlockSpec((1, tile), lambda i: (0, i)),
            pl.BlockSpec((1, tile), lambda i: (0, i)),
            whole,
        ],
        out_specs=pl.BlockSpec((PAIR, channels + 8, tokens // PAIR), lambda i: (0, 0, 0)),
        out_shape=jax.ShapeDtypeStruct((PAIR, channels + 8, tokens // PAIR), jnp.float32),
        scratch_shapes=[
            pltpu.VMEM((tokens, depth), jnp.bfloat16),
            pltpu.VMEM((width // tile, tokens, tile), jnp.float32),
            pltpu.VMEM((tokens, 1), jnp.float32),
        ],
        cost_estimate=pl.CostEstimate(
            flops=2 * tokens * width * (depth + 2 * channels),
            bytes_accessed=2 * width * depth,
            transcendentals=0,
        ),
        name="finish",
    )(
        attended,
        out_weight,
        latent,
        embed_rows,
        embed_bias.reshape(1, width),
        gate.reshape(1, width),
        final_weight,
    )


def prefix_over_steps(drift):
    half = jnp.bfloat16

    def wide(value):
        return value.astype(jnp.float32)

    other = wide(swap_cores(drift.astype(half)))
    within = jnp.where(lax.axis_index("core") == 1, other, jnp.zeros_like(other))
    here = drift + other
    near = wide(shift(here.astype(half), "chip", 1, False))
    near = near + wide(shift((here + near).astype(half), "chip", 2, False))
    window = (here + near).astype(half)
    chips = lax.axis_size("chip")
    far = send_by_core(window, 4, chips - 4, False)
    far = wide(far) + wide(send_by_core(far, 4, None, False))
    return within + near + far + wide(swap_cores(far.astype(half)))


def per_device(
    latent_old,
    noise_start,
    step_index,
    sigma_table,
    mod_weight,
    embed_weight,
    embed_bias,
    query_weight,
    query_gain,
    stale_keys,
    stale_values,
    out_weight,
    final_weight,
):
    parts, part = lax.axis_size("patch"), lax.axis_index("patch")
    width = embed_weight.shape[1]
    columns = query_weight.shape[1] // parts
    latent = latent_old[0].T
    channels, token_count = latent.shape
    key_rows = stale_keys.shape[1]

    core = lax.axis_index("core")
    kind = lax.rem(part, PAIR)
    first_part = part - kind

    def of_kind(rows):
        rows = rows.reshape(-1, CORES, out_weight.shape[0], *rows.shape[1:])
        return lax.dynamic_index_in_dim(rows, kind, 1, keepdims=False).reshape(-1, *rows.shape[3:])

    def embed(latent, embed_weight, embed_bias):
        hidden = lax.dot_general(
            latent.astype(jnp.bfloat16),
            embed_weight,
            (((0,), (0,)), ((), ())),
            preferred_element_type=jnp.float32,
        )
        hidden = hidden + embed_bias
        row_mean = jnp.mean(hidden, axis=-1, keepdims=True)
        row_var = jnp.mean(jnp.square(hidden - row_mean), axis=-1)
        return jnp.sqrt(row_var + epsilon)[None]

    def modulation(step_index, sigma_table, mod_weight):
        slots = jnp.arange(sigma_table.shape[0])
        sigma_now = jnp.sum(jnp.where(slots == step_index[0], sigma_table, 0.0))
        sigma_next = jnp.sum(jnp.where(slots == step_index[0] + 1, sigma_table, 0.0))
        embedded = jax.nn.silu(time_embed(sigma_now, mod_weight.shape[0] // 2)).astype(jnp.bfloat16)
        modulate = jnp.dot(embedded[None, :], mod_weight, preferred_element_type=jnp.float32)[0]
        return modulate, sigma_next - sigma_now

    def split(value):
        coarse = value.astype(jnp.bfloat16)
        return jnp.concatenate([coarse, (value - coarse.astype(jnp.float32)).astype(jnp.bfloat16)])

    def sources(modulate, embed_weight, embed_bias):
        shift_vec, scale_vec = modulate[:width], modulate[width : 2 * width]
        weight = embed_weight.astype(jnp.float32)
        centered = jnp.concatenate(
            [
                weight - jnp.mean(weight, axis=-1, keepdims=True),
                (embed_bias - jnp.mean(embed_bias))[None],
            ]
        )
        rows = [
            centered * (1.0 + scale_vec),
            shift_vec[None],
            shift_vec[None],
            jnp.zeros((EXTRA - 3, width), jnp.float32),
        ]
        return split(jnp.concatenate(rows))

    def features(modulate, embed_weight, embed_bias, final_weight):
        return (
            of_kind(embed_weight.T),
            of_kind(embed_bias),
            of_kind(modulate[2 * width :]),
            of_kind(final_weight),
        )

    my_columns = lax.dynamic_slice_in_dim(query_weight, part * columns, columns, 1)
    tasks = {
        1: (embed, (latent, embed_weight, embed_bias)),
        2: (
            functools.partial(pack, parts=parts),
            lambda done: (stale_keys[0], stale_values[0], latent, done[1]),
        ),
        4: (modulation, (step_index, sigma_table, mod_weight)),
        6: (sources, lambda done: (done[4][0], embed_weight, embed_bias)),
        7: (features, lambda done: (done[4][0], embed_weight, embed_bias, final_weight)),
    }
    other = swap_cores(my_columns)
    both = [jnp.where(core == 0, my_columns, other), jnp.where(core == 0, other, my_columns)]
    out_rows = jnp.where(core == kind, out_weight, swap_cores(out_weight))
    (gathered, out_rows), done = gather_rows((jnp.concatenate(both), out_rows), tasks)
    (modulate, delta), source, parameters = done[4], done[6], done[7]
    packed = lax.all_to_all(done[2], "patch", 0, 0, tiled=True)

    project = jnp.dot(source, gathered.reshape(width, columns), preferred_element_type=jnp.float32)
    deep = channels + EXTRA
    project = split(project[:deep] + project[deep:])
    project = jnp.moveaxis(project.reshape(2 * deep, -1, HEAD), 1, 0)
    row = lax.broadcasted_iota(jnp.int32, (1, 2 * deep, HEAD), 1)
    picks = jnp.where((row == channels + 1) | (row == channels + 2), 1.0, 0.0).astype(jnp.bfloat16)
    project = jnp.concatenate([project, jnp.broadcast_to(picks, project.shape)], axis=2)

    attended = attention(project, query_gain, packed, key_rows, token_count)
    attended = lax.all_to_all(attended, "patch", 0, 0, tiled=True)
    latents = lax.dynamic_slice_in_dim(packed, first_part, PAIR, 0)
    latents = latents[:, 2 * key_rows : 2 * key_rows + channels, :token_count]
    partial = finish(attended, out_rows.reshape(-1, out_rows.shape[2]), latents, *parameters)
    theirs = lax.dynamic_index_in_dim(partial, 1 - kind, 0, keepdims=False)
    mine = lax.dynamic_index_in_dim(partial, kind, 0, keepdims=False)
    theirs = lax.ppermute(theirs, "patch", [(p, p ^ 1) for p in range(parts)])
    between = 0.5 * (theirs[channels] - mine[channels])
    squares = mine[channels + 1] + theirs[channels + 1] + width * (between * between)
    here_sum = jnp.sum(parameters[3].astype(jnp.float32), axis=0)
    all_sum = jnp.sum(final_weight.astype(jnp.float32), axis=0)
    lean = (all_sum - 2.0 * here_sum)[:, None] * between
    scale = delta * lax.rsqrt(squares / width + epsilon)
    drift = (mine[:channels] + theirs[:channels] + lean) * scale
    return (noise_start.T + (prefix_over_steps(drift) + drift)).T[None]


def solution(mesh):
    shape = mesh.shape
    torus = Mesh(
        mesh.devices.reshape(shape["rep"], shape["step"] // CORES, CORES, shape["patch"]),
        ("rep", "chip", "core", "patch"),
    )
    placed = (
        P(REP_STEP, "patch", None),
        P(("rep", "patch"), None),
        P(REP_STEP),
        P(),
        P(),
        P(),
        P(),
        P(STEP, None),
        P(),
        P(REP_STEP, "patch", None),
        P(REP_STEP, "patch", None),
        P(STEP, None),
        P(),
    )
    return jax.shard_map(
        per_device,
        mesh=torus,
        in_specs=placed,
        out_specs=P(REP_STEP, "patch", None),
        check_vma=False,
    )
```

```python
import functools
import math

import jax
import jax.numpy as jnp
from jax import lax
from jax.experimental import pallas as pl
from jax.experimental.pallas import tpu as pltpu
from jax.sharding import Mesh
from jax.sharding import PartitionSpec as P

HEAD = 128
CORES = 2
EXTRA = 16
GATHER_AFTER = 2
STEP = ("chip", "core")
REP_STEP = ("rep", "chip", "core")
epsilon = 1e-06


def shift(value, axis, distance, wrap):
    size = lax.axis_size(axis)
    pairs = [(i, (i + distance) % size) for i in range(size) if wrap or 0 <= i + distance < size]
    return lax.ppermute(value, axis, pairs)


def swap_cores(value):
    return lax.ppermute(value, "core", [(0, 1), (1, 0)])


def send_by_core(value, first, second, wrap):
    chips = lax.axis_size("chip")
    pairs = []
    for core, distance in enumerate((first, second)):
        for chip in range(chips):
            target = chip + (distance or 0)
            if distance is not None and (wrap or 0 <= target < chips):
                pairs.append((chip * CORES + core, target % chips * CORES + core))
    return lax.ppermute(value, ("chip", "core"), pairs)


def project_body(chips, order_ref, source_ref, *refs):
    pieces, out_ref = refs[:-1], refs[-1]
    total = jnp.zeros((source_ref.shape[1], out_ref.shape[2]), jnp.float32)
    for k, piece in enumerate(pieces):
        product = jnp.dot(
            source_ref[order_ref[k]], piece[...], preferred_element_type=jnp.float32
        )
        total += jnp.where(order_ref[len(pieces) + k] == 1, product, 0.0)
    deep = out_ref.shape[1]
    for i in range(2):
        out_ref[i] = total[2 * i * deep : (2 * i + 1) * deep] + total[(2 * i + 1) * deep : (2 * i + 2) * deep]


def project_rows(source, pieces, owners, used):
    chips, height, rows = source.shape
    columns = pieces[0].shape[1]
    order = jnp.stack(owners + [u.astype(jnp.int32) for u in used])
    whole = pl.BlockSpec(memory_space=pltpu.VMEM)
    return pl.pallas_call(
        functools.partial(project_body, chips),
        in_specs=[pl.BlockSpec(memory_space=pltpu.SMEM), whole] + [whole] * len(pieces),
        out_specs=whole,
        out_shape=jax.ShapeDtypeStruct((2, height // 4, columns), jnp.float32),
        cost_estimate=pl.CostEstimate(
            flops=2 * len(pieces) * height * rows * columns,
            bytes_accessed=len(pieces) * rows * (2 * columns + 2 * height),
            transcendentals=0,
        ),
        name="project",
    )(order, source, *pieces)


def pass_round(piece, tasks):
    chips, here = lax.axis_size("chip"), lax.axis_index("chip")
    step = jnp.where(lax.axis_index("core") == 0, 1, -1)
    pieces, results = [piece], {}
    owners = [lax.rem(here - hop * step + chips, chips) for hop in range(chips // 2 + 1)]
    for hop in range(1, chips // 2 + 1):
        sent = send_by_core(piece, 1, -1, True)
        if hop in tasks:
            task, inputs = tasks[hop]
            if callable(inputs):
                inputs = inputs(results, pieces, owners)
            _, inputs = lax.optimization_barrier((piece, inputs))
            results[hop] = task(*inputs)
            sent, results[hop] = lax.optimization_barrier((sent, results[hop]))
        piece = sent
        pieces.append(piece)
    return pieces, owners, results


def time_embed(sigma_now, half_count):
    frequency = jnp.exp(
        -math.log(10000.0) * jnp.arange(half_count).astype(jnp.float32) / half_count
    )
    angles = 1000.0 * sigma_now * frequency
    return jnp.concatenate([jnp.cos(angles), jnp.sin(angles)])


def pack_body(key_ref, value_ref, latent_ref, spread_ref, out_ref):
    rows = key_ref.shape[0]
    channels, tokens = latent_ref.shape
    out_ref[0, :rows] = key_ref[...]
    out_ref[0, rows : 2 * rows] = value_ref[...]
    spread = spread_ref[...]
    coarse = spread.astype(jnp.bfloat16).astype(jnp.float32)
    tail = jnp.concatenate(
        [
            latent_ref[...],
            jnp.ones_like(spread),
            coarse,
            spread - coarse,
            jnp.zeros((EXTRA - 3, tokens), jnp.float32),
        ]
    )
    out_ref[0, 2 * rows :] = jnp.zeros((channels + EXTRA, out_ref.shape[2]), jnp.bfloat16)
    out_ref[0, 2 * rows :, :tokens] = tail.astype(jnp.bfloat16)


def pack(keys, values, latent, spread, parts):
    rows, width = keys.shape
    channels, tokens = latent.shape
    columns = width // parts
    height = 2 * rows + channels + EXTRA
    return pl.pallas_call(
        pack_body,
        grid=(parts,),
        in_specs=[
            pl.BlockSpec((rows, columns), lambda p: (0, p)),
            pl.BlockSpec((rows, columns), lambda p: (0, p)),
            pl.BlockSpec((channels, tokens), lambda p: (0, 0)),
            pl.BlockSpec((1, tokens), lambda p: (0, 0)),
        ],
        out_specs=pl.BlockSpec((1, height, columns), lambda p: (p, 0, 0)),
        out_shape=jax.ShapeDtypeStruct((parts, height, columns), jnp.bfloat16),
        cost_estimate=pl.CostEstimate(
            flops=parts * height * columns,
            bytes_accessed=4 * parts * height * columns,
            transcendentals=0,
        ),
        name="pack",
    )(keys, values, latent, spread)


def attention_body(parts, rows, packed_ref, project_ref, gain_ref, out_ref, even_ref, odd_ref):
    at, last = pl.program_id(0), pl.num_programs(0) - 2
    now, past = jnp.minimum(at, last), jnp.maximum(at - 1, 0)
    tile = even_ref.shape[0]
    head, part = now // parts, lax.rem(now, parts)

    def columns(head):
        return pl.ds(pl.multiple_of(head * HEAD, HEAD), HEAD)

    def run(now_ref, past_ref):
        tokens = packed_ref[part, 2 * rows :, :tile]
        both = lax.dot_general(
            jnp.concatenate([tokens, tokens]),
            project_ref[head],
            (((0,), (0,)), ((), ())),
            preferred_element_type=jnp.float32,
        )
        raw, spread = both[:, :HEAD], both[:, HEAD:]
        square = jnp.mean(raw * raw, axis=-1, keepdims=True) + epsilon * (spread * spread)
        queries = (raw * lax.rsqrt(square) * gain_ref[...]).astype(jnp.bfloat16)
        keys = packed_ref[:, :rows, columns(head)].reshape(-1, HEAD)
        now_ref[...] = lax.dot_general(
            queries, keys, (((1,), (1,)), ((), ())), preferred_element_type=jnp.float32
        )
        peak = jnp.max(past_ref[...], axis=-1, keepdims=True)
        weights = jnp.exp((past_ref[...] - peak) * (1.0 / math.sqrt(HEAD)))
        total = jnp.sum(weights, axis=-1, keepdims=True)
        values = packed_ref[:, rows : 2 * rows, columns(past // parts)].reshape(-1, HEAD)
        blended = jnp.dot(weights.astype(jnp.bfloat16), values, preferred_element_type=jnp.float32)
        out_ref[...] = (blended / total).astype(jnp.bfloat16)

    @pl.when(lax.rem(at, 2) == 0)
    def _():
        run(even_ref, odd_ref)

    @pl.when(lax.rem(at, 2) == 1)
    def _():
        run(odd_ref, even_ref)


def attention(project, query_gain, packed, rows, tile):
    parts, height, width = packed.shape
    tokens = parts * tile
    heads = width // HEAD
    work = tokens * parts * rows * width

    def past(i):
        at = jnp.maximum(i - 1, 0)
        return lax.rem(at, parts), at // parts

    whole = pl.BlockSpec(memory_space=pltpu.VMEM)
    return pl.pallas_call(
        functools.partial(attention_body, parts, rows),
        grid=(heads * parts + 1,),
        in_specs=[whole, whole, whole],
        out_specs=pl.BlockSpec((tile, HEAD), past),
        out_shape=jax.ShapeDtypeStruct((tokens, width), jnp.bfloat16),
        scratch_shapes=[pltpu.VMEM((tile, parts * rows), jnp.float32)] * 2,
        cost_estimate=pl.CostEstimate(
            flops=4 * work,
            bytes_accessed=4 * parts * rows * width + 6 * tokens * width,
            transcendentals=work // HEAD,
        ),
        name="attention",
    )(packed, project, query_gain.reshape(1, HEAD))


def finish_body(
    tile, attended_ref, weight_ref, hidden_ref, gate_ref, final_ref, delta_ref, out_ref, joined_ref, mixed_ref, sum_ref
):
    at = pl.program_id(0)
    parts, _, columns = attended_ref.shape

    @pl.when(at == 0)
    def _():
        for p in range(parts):
            joined_ref[:, p * columns : (p + 1) * columns] = attended_ref[p]
        sum_ref[...] = jnp.zeros_like(sum_ref)

    branch = lax.dot_general(
        weight_ref[...], joined_ref[...], (((1,), (1,)), ((), ())), preferred_element_type=jnp.float32
    )
    mixed = hidden_ref[pl.ds(pl.multiple_of(at * tile, tile), tile)] + gate_ref[...] * branch
    mixed_ref[at] = mixed
    sum_ref[...] += jnp.sum(mixed, axis=0, keepdims=True)

    @pl.when(at == pl.num_programs(0) - 1)
    def _():
        count = mixed_ref.shape[0]
        width = count * tile
        mean = sum_ref[...] / width
        squares = jnp.zeros_like(mean)
        for i in range(count):
            squares += jnp.sum(jnp.square(mixed_ref[i] - mean), axis=0, keepdims=True)
        scale = lax.rsqrt(squares / width + epsilon)
        velocity = jnp.zeros(out_ref.shape, jnp.float32)
        for i in range(count):
            velocity += jnp.dot(
                final_ref[:, i * tile : (i + 1) * tile],
                ((mixed_ref[i] - mean) * scale).astype(jnp.bfloat16),
                preferred_element_type=jnp.float32,
            )
        out_ref[...] = velocity * delta_ref[0]


def finish(attended, out_weight, hidden, gate, final_weight, delta):
    parts, tokens, columns = attended.shape
    width, depth = out_weight.shape
    channels = final_weight.shape[1]
    tile = min(512, width)
    whole = pl.BlockSpec(memory_space=pltpu.VMEM)
    return pl.pallas_call(
        functools.partial(finish_body, tile),
        grid=(width // tile,),
        in_specs=[
            whole,
            pl.BlockSpec((tile, depth), lambda i: (i, 0)),
            whole,
            pl.BlockSpec((tile, 1), lambda i: (i, 0)),
            whole,
            pl.BlockSpec(memory_space=pltpu.SMEM),
        ],
        out_specs=whole,
        out_shape=jax.ShapeDtypeStruct((channels, tokens), jnp.float32),
        scratch_shapes=[
            pltpu.VMEM((tokens, depth), jnp.bfloat16),
            pltpu.VMEM((width // tile, tile, tokens), jnp.float32),
            pltpu.VMEM((1, tokens), jnp.float32),
        ],
        cost_estimate=pl.CostEstimate(
            flops=2 * tokens * width * (depth + channels),
            bytes_accessed=2 * width * depth + 4 * tokens * width,
            transcendentals=0,
        ),
        name="finish",
    )(attended, out_weight, hidden, gate.reshape(width, 1), final_weight.T, delta.reshape(1))


def prefix_over_steps(drift):
    half = jnp.bfloat16

    def wide(value):
        return value.astype(jnp.float32)

    other = wide(swap_cores(drift.astype(half)))
    within = jnp.where(lax.axis_index("core") == 1, other, jnp.zeros_like(other))
    here = drift + other
    near = wide(shift(here.astype(half), "chip", 1, False))
    near = near + wide(shift((here + near).astype(half), "chip", 2, False))
    window = (here + near).astype(half)
    chips = lax.axis_size("chip")
    far = send_by_core(window, 4, chips - 4, False)
    far = wide(far) + wide(send_by_core(far, 4, None, False))
    return within + near + far + wide(swap_cores(far.astype(half)))


def per_device(
    latent_old,
    noise_start,
    step_index,
    sigma_table,
    mod_weight,
    embed_weight,
    embed_bias,
    query_weight,
    query_gain,
    stale_keys,
    stale_values,
    out_weight,
    final_weight,
):
    parts, part = lax.axis_size("patch"), lax.axis_index("patch")
    width = embed_weight.shape[1]
    columns = query_weight.shape[1] // parts
    latent = latent_old[0].T
    channels, token_count = latent.shape
    key_rows = stale_keys.shape[1]

    core = lax.axis_index("core")

    def embed(latent, embed_weight, embed_bias):
        hidden = lax.dot_general(
            embed_weight,
            latent.astype(jnp.bfloat16),
            (((0,), (0,)), ((), ())),
            preferred_element_type=jnp.float32,
        )
        hidden = hidden + embed_bias[:, None]
        mean = jnp.mean(hidden, axis=0, keepdims=True)
        variance = jnp.mean(jnp.square(hidden - mean), axis=0, keepdims=True)
        return hidden, jnp.sqrt(variance + epsilon)

    def levels(step_index, sigma_table):
        slots = jnp.arange(sigma_table.shape[0])
        sigma_now = jnp.sum(jnp.where(slots == step_index[0], sigma_table, 0.0))
        sigma_next = jnp.sum(jnp.where(slots == step_index[0] + 1, sigma_table, 0.0))
        return sigma_now, sigma_next - sigma_now

    def modulation(sigma_now, sigma_other, mod_weight):
        embedded = [time_embed(s, mod_weight.shape[0] // 2) for s in (sigma_now, sigma_other)]
        embedded = jax.nn.silu(jnp.stack(embedded)).astype(jnp.bfloat16)
        return jnp.dot(embedded, mod_weight, preferred_element_type=jnp.float32)

    def sources(modulate, embed_weight, embed_bias):
        weight = embed_weight.astype(jnp.float32)
        centered = jnp.concatenate(
            [
                weight - jnp.mean(weight, axis=-1, keepdims=True),
                (embed_bias - jnp.mean(embed_bias))[None],
                jnp.zeros((EXTRA - 1, width), jnp.float32),
            ]
        )
        row = lax.broadcasted_iota(jnp.int32, (centered.shape[0], 1), 0)
        shifted = (row == channels + 1) | (row == channels + 2)
        rows = []
        for i in range(CORES):
            shift_vec, scale_vec = modulate[i, :width], modulate[i, width : 2 * width]
            value = jnp.where(shifted, shift_vec, centered * (1.0 + scale_vec))
            coarse = value.astype(jnp.bfloat16)
            rows += [coarse, (value - coarse.astype(jnp.float32)).astype(jnp.bfloat16)]
        rows = jnp.concatenate(rows)
        return jnp.moveaxis(rows.reshape(rows.shape[0], lax.axis_size("chip"), -1), 1, 0)

    def split(value):
        coarse = value.astype(jnp.bfloat16)
        return jnp.concatenate([coarse, (value - coarse.astype(jnp.float32)).astype(jnp.bfloat16)])

    def first_pieces(done, pieces, owners):
        ready = pieces[: last_hop - 1]
        return done[6], ready, owners[: len(ready)], [core == 0] + [core >= 0] * (len(ready) - 1)

    my_columns = lax.dynamic_slice_in_dim(query_weight, part * columns, columns, 1)
    sigma_now, delta = levels(step_index, sigma_table)
    sigma_other = swap_cores(jnp.full((8, HEAD), sigma_now))[0, 0]
    other = swap_cores(my_columns)
    piece = [jnp.where(core == 0, my_columns, other), jnp.where(core == 0, other, my_columns)]
    last_hop = lax.axis_size("chip") // 2
    tasks = {
        1: (embed, (latent, embed_weight, embed_bias)),
        2: (
            functools.partial(pack, parts=parts),
            lambda done, *_: (stale_keys[0], stale_values[0], latent, done[1][1]),
        ),
        4: (modulation, (sigma_now, sigma_other, mod_weight)),
        6: (sources, lambda done, *_: (done[4], embed_weight, embed_bias)),
        last_hop: (project_rows, first_pieces),
    }
    pieces, owners, done = pass_round(jnp.concatenate(piece), tasks)
    hidden, modulate, source = done[1][0], done[4][0], done[6]
    packed = lax.all_to_all(done[2], "patch", 0, 0, tiled=True)
    _, late = lax.optimization_barrier((pieces[GATHER_AFTER], out_weight))
    all_out_weight = lax.all_gather(late, STEP, axis=0, tiled=True)

    deep = channels + EXTRA
    shares = done[last_hop] + project_rows(
        source, pieces[-2:], owners[-2:], [core >= 0, core == 1]
    )
    project = split(shares[0] + swap_cores(shares[1]))
    project = jnp.moveaxis(project.reshape(2 * deep, -1, HEAD), 1, 0)
    row = lax.broadcasted_iota(jnp.int32, (1, 2 * deep, HEAD), 1)
    picks = jnp.where((row == channels + 1) | (row == channels + 2), 1.0, 0.0).astype(jnp.bfloat16)
    project = jnp.concatenate([project, jnp.broadcast_to(picks, project.shape)], axis=2)

    attended = attention(project, query_gain, packed, key_rows, token_count)
    attended = lax.all_to_all(
        attended.reshape(parts, token_count, columns), "patch", 0, 0, tiled=True
    )
    drift = finish(attended, all_out_weight, hidden, modulate[2 * width :], final_weight, delta)
    return (noise_start.T + (prefix_over_steps(drift) + drift)).T[None]


def solution(mesh):
    shape = mesh.shape
    torus = Mesh(
        mesh.devices.reshape(shape["rep"], shape["step"] // CORES, CORES, shape["patch"]),
        ("rep", "chip", "core", "patch"),
    )
    placed = (
        P(REP_STEP, "patch", None),
        P(("rep", "patch"), None),
        P(REP_STEP),
        P(),
        P(),
        P(),
        P(),
        P(STEP, None),
        P(),
        P(REP_STEP, "patch", None),
        P(REP_STEP, "patch", None),
        P(STEP, None),
        P(),
    )
    return jax.shard_map(
        per_device,
        mesh=torus,
        in_specs=placed,
        out_specs=P(REP_STEP, "patch", None),
        check_vma=False,
    )
```

```python
import functools
import math

import jax
import jax.numpy as jnp
from jax import lax
from jax.experimental import pallas as pl
from jax.experimental.pallas import tpu as pltpu
from jax.sharding import Mesh
from jax.sharding import PartitionSpec as P

HEAD = 128
CORES = 2
EXTRA = 16
STEP = ("chip", "core")
REP_STEP = ("rep", "chip", "core")
epsilon = 1e-06


def shift(value, axis, distance, wrap):
    size = lax.axis_size(axis)
    pairs = [(i, (i + distance) % size) for i in range(size) if wrap or 0 <= i + distance < size]
    return lax.ppermute(value, axis, pairs)


def swap_cores(value):
    return lax.ppermute(value, "core", [(0, 1), (1, 0)])


def send_by_core(value, first, second, wrap):
    chips = lax.axis_size("chip")
    pairs = []
    for core, distance in enumerate((first, second)):
        for chip in range(chips):
            target = chip + (distance or 0)
            if distance is not None and (wrap or 0 <= target < chips):
                pairs.append((chip * CORES + core, target % chips * CORES + core))
    return lax.ppermute(value, ("chip", "core"), pairs)


def gather_rows(shard, tasks):
    chips, here, core = lax.axis_size("chip"), lax.axis_index("chip"), lax.axis_index("core")
    other = swap_cores(shard)
    piece = jnp.concatenate([jnp.where(core == 0, shard, other), jnp.where(core == 0, other, shard)])
    rows = piece.shape[0]
    step = jnp.where(core == 0, 1, -1)
    half = chips // 2
    pieces, waiting, results = [(0, piece)], [], {}
    for hop in range(1, half + 1):
        sent = send_by_core(piece, 1, -1, True)
        if hop in tasks:
            task, inputs = tasks[hop]
            if callable(inputs):
                inputs = inputs(results)
            _, inputs = lax.optimization_barrier((piece, inputs))
            results[hop] = task(*inputs)
            sent, results[hop] = lax.optimization_barrier((sent, results[hop]))
        piece = sent
        pieces.append((hop, piece))
        if 2 * hop != chips:
            waiting.append((hop, piece))
        if hop in (half // 2, half - 1):
            swapped = swap_cores(jnp.concatenate([p for _, p in waiting]))
            for i, (at, _) in enumerate(waiting):
                pieces.append((-at, swapped[i * rows : (i + 1) * rows]))
            waiting = []
    held = jnp.zeros((chips, *piece.shape), shard.dtype)
    for at, piece in pieces:
        owner = lax.rem(here - at * step + chips, chips)
        held = lax.dynamic_update_slice_in_dim(held, piece[None], owner, 0)
    return held, results


def time_embed(sigma_now, half_count):
    frequency = jnp.exp(
        -math.log(10000.0) * jnp.arange(half_count).astype(jnp.float32) / half_count
    )
    angles = 1000.0 * sigma_now * frequency
    return jnp.concatenate([jnp.cos(angles), jnp.sin(angles)])


def pack_body(key_ref, value_ref, latent_ref, spread_ref, out_ref):
    rows = key_ref.shape[0]
    channels, tokens = latent_ref.shape
    out_ref[0, :rows] = key_ref[...]
    out_ref[0, rows : 2 * rows] = value_ref[...]
    spread = spread_ref[...]
    coarse = spread.astype(jnp.bfloat16).astype(jnp.float32)
    tail = jnp.concatenate(
        [
            latent_ref[...],
            jnp.ones_like(spread),
            coarse,
            spread - coarse,
            jnp.zeros((EXTRA - 3, tokens), jnp.float32),
        ]
    )
    out_ref[0, 2 * rows :] = jnp.zeros((channels + EXTRA, out_ref.shape[2]), jnp.bfloat16)
    out_ref[0, 2 * rows :, :tokens] = tail.astype(jnp.bfloat16)


def pack(keys, values, latent, spread, parts):
    rows, width = keys.shape
    channels, tokens = latent.shape
    columns = width // parts
    height = 2 * rows + channels + EXTRA
    return pl.pallas_call(
        pack_body,
        grid=(parts,),
        in_specs=[
            pl.BlockSpec((rows, columns), lambda p: (0, p)),
            pl.BlockSpec((rows, columns), lambda p: (0, p)),
            pl.BlockSpec((channels, tokens), lambda p: (0, 0)),
            pl.BlockSpec((1, tokens), lambda p: (0, 0)),
        ],
        out_specs=pl.BlockSpec((1, height, columns), lambda p: (p, 0, 0)),
        out_shape=jax.ShapeDtypeStruct((parts, height, columns), jnp.bfloat16),
        cost_estimate=pl.CostEstimate(
            flops=parts * height * columns,
            bytes_accessed=4 * parts * height * columns,
            transcendentals=0,
        ),
        name="pack",
    )(keys, values, latent, spread)


def attention_body(parts, rows, tile, packed_ref, project_ref, gain_ref, out_ref):
    columns = pl.ds(pl.multiple_of(pl.program_id(0) * HEAD, HEAD), HEAD)
    keys = packed_ref[:, :rows, columns].reshape(-1, HEAD)
    values = packed_ref[:, rows : 2 * rows, columns].reshape(-1, HEAD)
    queries = []
    for part in range(parts):
        tokens = packed_ref[part, 2 * rows :, :tile]
        both = lax.dot_general(
            jnp.concatenate([tokens, tokens]),
            project_ref[0],
            (((0,), (0,)), ((), ())),
            preferred_element_type=jnp.float32,
        )
        raw, spread = both[:, :HEAD], both[:, HEAD:]
        square = jnp.mean(raw * raw, axis=-1, keepdims=True) + epsilon * (spread * spread)
        queries.append((raw * lax.rsqrt(square) * gain_ref[...]).astype(jnp.bfloat16))
    scores = [
        lax.dot_general(q, keys, (((1,), (1,)), ((), ())), preferred_element_type=jnp.float32)
        for q in queries
    ]
    for part in range(parts):
        peak = jnp.max(scores[part], axis=-1, keepdims=True)
        weights = jnp.exp((scores[part] - peak) * (1.0 / math.sqrt(HEAD)))
        total = jnp.sum(weights, axis=-1, keepdims=True)
        blended = jnp.dot(weights.astype(jnp.bfloat16), values, preferred_element_type=jnp.float32)
        out_ref[part] = (blended / total).astype(jnp.bfloat16)


def attention(project, query_gain, packed, rows, tile):
    parts, height, width = packed.shape
    tokens = parts * tile
    heads = width // HEAD
    work = tokens * parts * rows * width
    whole = pl.BlockSpec(memory_space=pltpu.VMEM)
    return pl.pallas_call(
        functools.partial(attention_body, parts, rows, tile),
        grid=(heads,),
        in_specs=[whole, pl.BlockSpec((1, *project.shape[1:]), lambda h: (h, 0, 0)), whole],
        out_specs=pl.BlockSpec((parts, tile, HEAD), lambda h: (0, 0, h)),
        out_shape=jax.ShapeDtypeStruct((parts, tile, width), jnp.bfloat16),
        cost_estimate=pl.CostEstimate(
            flops=4 * work,
            bytes_accessed=4 * parts * rows * width + 6 * tokens * width,
            transcendentals=work // HEAD,
        ),
        name="attention",
    )(packed, project, query_gain.reshape(1, HEAD))


def prefix_over_steps(drift):
    half = jnp.bfloat16

    def wide(value):
        return value.astype(jnp.float32)

    other = wide(swap_cores(drift.astype(half)))
    within = jnp.where(lax.axis_index("core") == 1, other, jnp.zeros_like(other))
    here = drift + other
    near = wide(shift(here.astype(half), "chip", 1, False))
    near = near + wide(shift((here + near).astype(half), "chip", 2, False))
    window = (here + near).astype(half)
    chips = lax.axis_size("chip")
    far = send_by_core(window, 4, chips - 4, False)
    far = wide(far) + wide(send_by_core(far, 4, None, False))
    return within + near + far + wide(swap_cores(far.astype(half)))


def per_device(
    latent_old,
    noise_start,
    step_index,
    sigma_table,
    mod_weight,
    embed_weight,
    embed_bias,
    query_weight,
    query_gain,
    stale_keys,
    stale_values,
    out_weight,
    final_weight,
):
    parts, part = lax.axis_size("patch"), lax.axis_index("patch")
    width = embed_weight.shape[1]
    columns = query_weight.shape[1] // parts
    latent = latent_old[0].T
    channels, token_count = latent.shape
    key_rows = stale_keys.shape[1]

    all_out_weight = lax.all_gather(out_weight, STEP, axis=0, tiled=True)

    def embed(latent, embed_weight, embed_bias):
        hidden = lax.dot_general(
            latent.astype(jnp.bfloat16),
            embed_weight,
            (((0,), (0,)), ((), ())),
            preferred_element_type=jnp.float32,
        )
        hidden = hidden + embed_bias
        row_mean = jnp.mean(hidden, axis=-1, keepdims=True)
        row_var = jnp.mean(jnp.square(hidden - row_mean), axis=-1)
        return hidden, jnp.sqrt(row_var + epsilon)[None]

    def modulation(step_index, sigma_table, mod_weight):
        slots = jnp.arange(sigma_table.shape[0])
        sigma_now = jnp.sum(jnp.where(slots == step_index[0], sigma_table, 0.0))
        sigma_next = jnp.sum(jnp.where(slots == step_index[0] + 1, sigma_table, 0.0))
        embedded = jax.nn.silu(time_embed(sigma_now, mod_weight.shape[0] // 2)).astype(jnp.bfloat16)
        modulate = jnp.dot(embedded[None, :], mod_weight, preferred_element_type=jnp.float32)[0]
        return modulate, sigma_next - sigma_now

    def split(value):
        coarse = value.astype(jnp.bfloat16)
        return jnp.concatenate([coarse, (value - coarse.astype(jnp.float32)).astype(jnp.bfloat16)])

    def sources(modulate, embed_weight, embed_bias):
        shift_vec, scale_vec = modulate[:width], modulate[width : 2 * width]
        weight = embed_weight.astype(jnp.float32)
        centered = jnp.concatenate(
            [
                weight - jnp.mean(weight, axis=-1, keepdims=True),
                (embed_bias - jnp.mean(embed_bias))[None],
            ]
        )
        rows = [
            centered * (1.0 + scale_vec),
            shift_vec[None],
            shift_vec[None],
            jnp.zeros((EXTRA - 3, width), jnp.float32),
        ]
        return split(jnp.concatenate(rows))

    my_columns = lax.dynamic_slice_in_dim(query_weight, part * columns, columns, 1)
    tasks = {
        1: (embed, (latent, embed_weight, embed_bias)),
        2: (
            functools.partial(pack, parts=parts),
            lambda done: (stale_keys[0], stale_values[0], latent, done[1][1]),
        ),
        4: (modulation, (step_index, sigma_table, mod_weight)),
        6: (sources, lambda done: (done[4][0], embed_weight, embed_bias)),
    }
    gathered, done = gather_rows(my_columns, tasks)
    hidden, (modulate, delta), source = done[1][0], done[4], done[6]
    packed = lax.all_to_all(done[2], "patch", 0, 0, tiled=True)

    project = jnp.dot(source, gathered.reshape(width, columns), preferred_element_type=jnp.float32)
    deep = channels + EXTRA
    project = split(project[:deep] + project[deep:])
    project = jnp.moveaxis(project.reshape(2 * deep, -1, HEAD), 1, 0)
    row = lax.broadcasted_iota(jnp.int32, (1, 2 * deep, HEAD), 1)
    picks = jnp.where((row == channels + 1) | (row == channels + 2), 1.0, 0.0).astype(jnp.bfloat16)
    project = jnp.concatenate([project, jnp.broadcast_to(picks, project.shape)], axis=2)

    attended = attention(project, query_gain, packed, key_rows, token_count)
    attended = lax.all_to_all(attended, "patch", 0, 0, tiled=True)
    attended = jnp.moveaxis(attended, 0, 1).reshape(token_count, -1)
    branch = lax.dot_general(
        attended, all_out_weight, (((1,), (1,)), ((), ())), preferred_element_type=jnp.float32
    )
    mixed = hidden + modulate[2 * width :] * branch
    centered = mixed - jnp.mean(mixed, axis=-1, keepdims=True)
    variance = jnp.mean(jnp.square(centered), axis=-1, keepdims=True)
    normed = (centered * lax.rsqrt(variance + epsilon)).astype(jnp.bfloat16)
    velocity = lax.dot_general(
        final_weight, normed, (((0,), (1,)), ((), ())), preferred_element_type=jnp.float32
    )
    drift = velocity * delta
    return (noise_start.T + (prefix_over_steps(drift) + drift)).T[None]


def solution(mesh):
    shape = mesh.shape
    torus = Mesh(
        mesh.devices.reshape(shape["rep"], shape["step"] // CORES, CORES, shape["patch"]),
        ("rep", "chip", "core", "patch"),
    )
    placed = (
        P(REP_STEP, "patch", None),
        P(("rep", "patch"), None),
        P(REP_STEP),
        P(),
        P(),
        P(),
        P(),
        P(STEP, None),
        P(),
        P(REP_STEP, "patch", None),
        P(REP_STEP, "patch", None),
        P(STEP, None),
        P(),
    )
    return jax.shard_map(
        per_device,
        mesh=torus,
        in_specs=placed,
        out_specs=P(REP_STEP, "patch", None),
        check_vma=False,
    )
```

```python
import functools
import math

import jax
import jax.numpy as jnp
from jax import lax
from jax.experimental import pallas as pl
from jax.experimental.pallas import tpu as pltpu
from jax.sharding import Mesh
from jax.sharding import PartitionSpec as P

HEAD = 128
CORES = 2
EXTRA = 16
STEP = ("chip", "core")
REP_STEP = ("rep", "chip", "core")
epsilon = 1e-06


def shift(value, axis, distance, wrap):
    size = lax.axis_size(axis)
    pairs = [(i, (i + distance) % size) for i in range(size) if wrap or 0 <= i + distance < size]
    return lax.ppermute(value, axis, pairs)


def swap_cores(value):
    return lax.ppermute(value, "core", [(0, 1), (1, 0)])


def send_by_core(value, first, second, wrap):
    chips = lax.axis_size("chip")
    pairs = []
    for core, distance in enumerate((first, second)):
        for chip in range(chips):
            target = chip + (distance or 0)
            if distance is not None and (wrap or 0 <= target < chips):
                pairs.append((chip * CORES + core, target % chips * CORES + core))
    return lax.ppermute(value, ("chip", "core"), pairs)


def pass_round(piece, tasks):
    half = lax.axis_size("chip") // 2
    own, swapped, waiting, results = [piece], [], [], {}
    for hop in range(1, half + 1):
        sent = send_by_core(piece, 1, -1, True)
        if hop in tasks:
            task, inputs = tasks[hop]
            if callable(inputs):
                inputs = inputs(results)
            _, inputs = lax.optimization_barrier((piece, inputs))
            results[hop] = task(*inputs)
            sent, results[hop] = lax.optimization_barrier((sent, results[hop]))
        piece = sent
        own.append(piece)
        waiting.append(piece)
        if hop in (half // 2, half - 1):
            swapped.append(swap_cores(jnp.concatenate(waiting)))
            waiting = []
    return own, swapped, results


def project_body(counts, place_ref, source_ref, *refs):
    own, swapped, out_ref, joined_ref = refs[:-4], refs[-4:-2], refs[-2], refs[-1]
    rows = own[0].shape[0]

    def put(value, slot):
        joined_ref[pl.ds(pl.multiple_of(place_ref[slot] * rows, rows), rows)] = value

    for hop, piece in enumerate(own):
        put(piece[...], hop)
    slot = len(own)
    for count, batch in zip(counts, swapped):
        for i in range(count):
            put(batch[i * rows : (i + 1) * rows], slot)
            slot += 1
    total = jnp.dot(source_ref[...], joined_ref[...], preferred_element_type=jnp.float32)
    deep = total.shape[0] // 2
    total = total[:deep] + total[deep:]
    coarse = total.astype(jnp.bfloat16)
    fine = (total - coarse.astype(jnp.float32)).astype(jnp.bfloat16)
    row = lax.broadcasted_iota(jnp.int32, (deep, HEAD), 0)
    spread = (row == deep - EXTRA + 1) | (row == deep - EXTRA + 2)
    picks = jnp.where(spread, 1.0, 0.0).astype(jnp.bfloat16)
    for head in range(out_ref.shape[0]):
        columns = slice(head * HEAD, (head + 1) * HEAD)
        out_ref[head, :deep, :HEAD] = coarse[:, columns]
        out_ref[head, deep:, :HEAD] = fine[:, columns]
        out_ref[head, :deep, HEAD:] = picks
        out_ref[head, deep:, HEAD:] = jnp.zeros_like(picks)


def project_latents(source, own, swapped):
    chips, here = lax.axis_size("chip"), lax.axis_index("chip")
    step = jnp.where(lax.axis_index("core") == 0, 1, -1)
    rows, columns = own[0].shape
    counts = [batch.shape[0] // rows for batch in swapped]
    hops = list(range(len(own))) + [-hop for hop in range(1, sum(counts) + 1)]
    places = lax.rem(here - jnp.array(hops, jnp.int32) * step + chips, chips)
    whole = pl.BlockSpec(memory_space=pltpu.VMEM)
    return pl.pallas_call(
        functools.partial(project_body, counts),
        in_specs=[pl.BlockSpec(memory_space=pltpu.SMEM)] + [whole] * (1 + len(own) + len(swapped)),
        out_specs=whole,
        out_shape=jax.ShapeDtypeStruct((columns // HEAD, source.shape[0], 2 * HEAD), jnp.bfloat16),
        scratch_shapes=[pltpu.VMEM((chips * rows, columns), jnp.bfloat16)],
        cost_estimate=pl.CostEstimate(
            flops=2 * source.size * columns,
            bytes_accessed=2 * source.size + 4 * chips * rows * columns,
            transcendentals=0,
        ),
        name="project",
    )(places, source, *own, *swapped)


def time_embed(sigma_now, half_count):
    frequency = jnp.exp(
        -math.log(10000.0) * jnp.arange(half_count).astype(jnp.float32) / half_count
    )
    angles = 1000.0 * sigma_now * frequency
    return jnp.concatenate([jnp.cos(angles), jnp.sin(angles)])


def pack_body(key_ref, value_ref, latent_ref, spread_ref, out_ref):
    rows = key_ref.shape[0]
    channels, tokens = latent_ref.shape
    out_ref[0, :rows] = key_ref[...]
    out_ref[0, rows : 2 * rows] = value_ref[...]
    spread = spread_ref[...]
    coarse = spread.astype(jnp.bfloat16).astype(jnp.float32)
    tail = jnp.concatenate(
        [
            latent_ref[...],
            jnp.ones_like(spread),
            coarse,
            spread - coarse,
            jnp.zeros((EXTRA - 3, tokens), jnp.float32),
        ]
    )
    out_ref[0, 2 * rows :] = jnp.zeros((channels + EXTRA, out_ref.shape[2]), jnp.bfloat16)
    out_ref[0, 2 * rows :, :tokens] = tail.astype(jnp.bfloat16)


def pack(keys, values, latent, spread, parts):
    rows, width = keys.shape
    channels, tokens = latent.shape
    columns = width // parts
    height = 2 * rows + channels + EXTRA
    return pl.pallas_call(
        pack_body,
        grid=(parts,),
        in_specs=[
            pl.BlockSpec((rows, columns), lambda p: (0, p)),
            pl.BlockSpec((rows, columns), lambda p: (0, p)),
            pl.BlockSpec((channels, tokens), lambda p: (0, 0)),
            pl.BlockSpec((1, tokens), lambda p: (0, 0)),
        ],
        out_specs=pl.BlockSpec((1, height, columns), lambda p: (p, 0, 0)),
        out_shape=jax.ShapeDtypeStruct((parts, height, columns), jnp.bfloat16),
        cost_estimate=pl.CostEstimate(
            flops=parts * height * columns,
            bytes_accessed=4 * parts * height * columns,
            transcendentals=0,
        ),
        name="pack",
    )(keys, values, latent, spread)


def attention_body(parts, rows, tile, packed_ref, project_ref, gain_ref, out_ref):
    columns = pl.ds(pl.multiple_of(pl.program_id(0) * HEAD, HEAD), HEAD)
    keys = packed_ref[:, :rows, columns].reshape(-1, HEAD)
    values = packed_ref[:, rows : 2 * rows, columns].reshape(-1, HEAD)
    queries = []
    for part in range(parts):
        tokens = packed_ref[part, 2 * rows :, :tile]
        both = lax.dot_general(
            jnp.concatenate([tokens, tokens]),
            project_ref[0],
            (((0,), (0,)), ((), ())),
            preferred_element_type=jnp.float32,
        )
        raw, spread = both[:, :HEAD], both[:, HEAD:]
        square = jnp.mean(raw * raw, axis=-1, keepdims=True) + epsilon * (spread * spread)
        queries.append((raw * lax.rsqrt(square) * gain_ref[...]).astype(jnp.bfloat16))
    scores = [
        lax.dot_general(q, keys, (((1,), (1,)), ((), ())), preferred_element_type=jnp.float32)
        for q in queries
    ]
    for part in range(parts):
        peak = jnp.max(scores[part], axis=-1, keepdims=True)
        weights = jnp.exp((scores[part] - peak) * (1.0 / math.sqrt(HEAD)))
        total = jnp.sum(weights, axis=-1, keepdims=True)
        blended = jnp.dot(weights.astype(jnp.bfloat16), values, preferred_element_type=jnp.float32)
        out_ref[part] = (blended / total).astype(jnp.bfloat16)


def attention(project, query_gain, packed, rows, tile):
    parts, height, width = packed.shape
    tokens = parts * tile
    heads = width // HEAD
    work = tokens * parts * rows * width
    whole = pl.BlockSpec(memory_space=pltpu.VMEM)
    return pl.pallas_call(
        functools.partial(attention_body, parts, rows, tile),
        grid=(heads,),
        in_specs=[whole, pl.BlockSpec((1, *project.shape[1:]), lambda h: (h, 0, 0)), whole],
        out_specs=pl.BlockSpec((parts, tile, HEAD), lambda h: (0, 0, h)),
        out_shape=jax.ShapeDtypeStruct((parts, tile, width), jnp.bfloat16),
        cost_estimate=pl.CostEstimate(
            flops=4 * work,
            bytes_accessed=4 * parts * rows * width + 6 * tokens * width,
            transcendentals=work // HEAD,
        ),
        name="attention",
    )(packed, project, query_gain.reshape(1, HEAD))


def prefix_over_steps(drift):
    half = jnp.bfloat16

    def wide(value):
        return value.astype(jnp.float32)

    other = wide(swap_cores(drift.astype(half)))
    within = jnp.where(lax.axis_index("core") == 1, other, jnp.zeros_like(other))
    here = drift + other
    near = wide(shift(here.astype(half), "chip", 1, False))
    near = near + wide(shift((here + near).astype(half), "chip", 2, False))
    window = (here + near).astype(half)
    chips = lax.axis_size("chip")
    far = send_by_core(window, 4, chips - 4, False)
    far = wide(far) + wide(send_by_core(far, 4, None, False))
    return within + near + far + wide(swap_cores(far.astype(half)))


def per_device(
    latent_old,
    noise_start,
    step_index,
    sigma_table,
    mod_weight,
    embed_weight,
    embed_bias,
    query_weight,
    query_gain,
    stale_keys,
    stale_values,
    out_weight,
    final_weight,
):
    parts, part = lax.axis_size("patch"), lax.axis_index("patch")
    width = embed_weight.shape[1]
    columns = query_weight.shape[1] // parts
    latent = latent_old[0].T
    channels, token_count = latent.shape
    key_rows = stale_keys.shape[1]

    core = lax.axis_index("core")

    all_out_weight = lax.all_gather(out_weight, STEP, axis=0, tiled=True)

    def embed(latent, embed_weight, embed_bias):
        hidden = lax.dot_general(
            latent.astype(jnp.bfloat16),
            embed_weight,
            (((0,), (0,)), ((), ())),
            preferred_element_type=jnp.float32,
        )
        hidden = hidden + embed_bias
        row_mean = jnp.mean(hidden, axis=-1, keepdims=True)
        row_var = jnp.mean(jnp.square(hidden - row_mean), axis=-1)
        return hidden, jnp.sqrt(row_var + epsilon)[None]

    def modulation(step_index, sigma_table, mod_weight):
        slots = jnp.arange(sigma_table.shape[0])
        sigma_now = jnp.sum(jnp.where(slots == step_index[0], sigma_table, 0.0))
        sigma_next = jnp.sum(jnp.where(slots == step_index[0] + 1, sigma_table, 0.0))
        embedded = jax.nn.silu(time_embed(sigma_now, mod_weight.shape[0] // 2)).astype(jnp.bfloat16)
        modulate = jnp.dot(embedded[None, :], mod_weight, preferred_element_type=jnp.float32)[0]
        return modulate, sigma_next - sigma_now

    def split(value):
        coarse = value.astype(jnp.bfloat16)
        return jnp.concatenate([coarse, (value - coarse.astype(jnp.float32)).astype(jnp.bfloat16)])

    def sources(modulate, embed_weight, embed_bias):
        shift_vec, scale_vec = modulate[:width], modulate[width : 2 * width]
        weight = embed_weight.astype(jnp.float32)
        centered = jnp.concatenate(
            [
                weight - jnp.mean(weight, axis=-1, keepdims=True),
                (embed_bias - jnp.mean(embed_bias))[None],
            ]
        )
        rows = [
            centered * (1.0 + scale_vec),
            shift_vec[None],
            shift_vec[None],
            jnp.zeros((EXTRA - 3, width), jnp.float32),
        ]
        return split(jnp.concatenate(rows))

    my_columns = lax.dynamic_slice_in_dim(query_weight, part * columns, columns, 1)
    tasks = {
        1: (embed, (latent, embed_weight, embed_bias)),
        2: (
            functools.partial(pack, parts=parts),
            lambda done: (stale_keys[0], stale_values[0], latent, done[1][1]),
        ),
        4: (modulation, (step_index, sigma_table, mod_weight)),
        6: (sources, lambda done: (done[4][0], embed_weight, embed_bias)),
    }
    other = swap_cores(my_columns)
    piece = [jnp.where(core == 0, my_columns, other), jnp.where(core == 0, other, my_columns)]
    own, swapped, done = pass_round(jnp.concatenate(piece), tasks)
    hidden, (modulate, delta), source = done[1][0], done[4], done[6]
    packed = lax.all_to_all(done[2], "patch", 0, 0, tiled=True)

    project = project_latents(source, own, swapped)
    attended = attention(project, query_gain, packed, key_rows, token_count)
    attended = lax.all_to_all(attended, "patch", 0, 0, tiled=True)
    attended = jnp.moveaxis(attended, 0, 1).reshape(token_count, -1)
    branch = lax.dot_general(
        attended, all_out_weight, (((1,), (1,)), ((), ())), preferred_element_type=jnp.float32
    )
    mixed = hidden + modulate[2 * width :] * branch
    centered = mixed - jnp.mean(mixed, axis=-1, keepdims=True)
    variance = jnp.mean(jnp.square(centered), axis=-1, keepdims=True)
    normed = (centered * lax.rsqrt(variance + epsilon)).astype(jnp.bfloat16)
    velocity = lax.dot_general(
        final_weight, normed, (((0,), (1,)), ((), ())), preferred_element_type=jnp.float32
    )
    drift = velocity * delta
    return (noise_start.T + (prefix_over_steps(drift) + drift)).T[None]


def solution(mesh):
    shape = mesh.shape
    torus = Mesh(
        mesh.devices.reshape(shape["rep"], shape["step"] // CORES, CORES, shape["patch"]),
        ("rep", "chip", "core", "patch"),
    )
    placed = (
        P(REP_STEP, "patch", None),
        P(("rep", "patch"), None),
        P(REP_STEP),
        P(),
        P(),
        P(),
        P(),
        P(STEP, None),
        P(),
        P(REP_STEP, "patch", None),
        P(REP_STEP, "patch", None),
        P(STEP, None),
        P(),
    )
    return jax.shard_map(
        per_device,
        mesh=torus,
        in_specs=placed,
        out_specs=P(REP_STEP, "patch", None),
        check_vma=False,
    )
```

```python
import functools
import math

import jax
import jax.numpy as jnp
from jax import lax
from jax.experimental import pallas as pl
from jax.experimental.pallas import tpu as pltpu
from jax.sharding import Mesh
from jax.sharding import PartitionSpec as P

HEAD = 128
CORES = 2
EXTRA = 16
GATHER_AFTER = 2
STEP = ("chip", "core")
REP_STEP = ("rep", "chip", "core")
epsilon = 1e-06


def shift(value, axis, distance, wrap):
    size = lax.axis_size(axis)
    pairs = [(i, (i + distance) % size) for i in range(size) if wrap or 0 <= i + distance < size]
    return lax.ppermute(value, axis, pairs)


def swap_cores(value):
    return lax.ppermute(value, "core", [(0, 1), (1, 0)])


def send_by_core(value, first, second, wrap):
    chips = lax.axis_size("chip")
    pairs = []
    for core, distance in enumerate((first, second)):
        for chip in range(chips):
            target = chip + (distance or 0)
            if distance is not None and (wrap or 0 <= target < chips):
                pairs.append((chip * CORES + core, target % chips * CORES + core))
    return lax.ppermute(value, ("chip", "core"), pairs)


def pass_round(piece, tasks):
    half = lax.axis_size("chip") // 2
    own, swapped, waiting, results = [piece], [], [], {}
    for hop in range(1, half + 1):
        sent = send_by_core(piece, 1, -1, True)
        if hop in tasks:
            task, inputs = tasks[hop]
            if callable(inputs):
                inputs = inputs(results)
            _, inputs = lax.optimization_barrier((piece, inputs))
            results[hop] = task(*inputs)
            sent, results[hop] = lax.optimization_barrier((sent, results[hop]))
        piece = sent
        own.append(piece)
        waiting.append(piece)
        if hop in (half // 2, half - 1):
            swapped.append(swap_cores(jnp.concatenate(waiting)))
            waiting = []
    return own, swapped, results


def project_body(counts, place_ref, source_ref, *refs):
    own, swapped, out_ref, joined_ref = refs[:-4], refs[-4:-2], refs[-2], refs[-1]
    rows = own[0].shape[0]

    def put(value, slot):
        joined_ref[pl.ds(pl.multiple_of(place_ref[slot] * rows, rows), rows)] = value

    for hop, piece in enumerate(own):
        put(piece[...], hop)
    slot = len(own)
    for count, batch in zip(counts, swapped):
        for i in range(count):
            put(batch[i * rows : (i + 1) * rows], slot)
            slot += 1
    total = jnp.dot(source_ref[...], joined_ref[...], preferred_element_type=jnp.float32)
    deep = total.shape[0] // 2
    total = total[:deep] + total[deep:]
    coarse = total.astype(jnp.bfloat16)
    fine = (total - coarse.astype(jnp.float32)).astype(jnp.bfloat16)
    row = lax.broadcasted_iota(jnp.int32, (deep, HEAD), 0)
    spread = (row == deep - EXTRA + 1) | (row == deep - EXTRA + 2)
    picks = jnp.where(spread, 1.0, 0.0).astype(jnp.bfloat16)
    for head in range(out_ref.shape[0]):
        columns = slice(head * HEAD, (head + 1) * HEAD)
        out_ref[head, :deep, :HEAD] = coarse[:, columns]
        out_ref[head, deep:, :HEAD] = fine[:, columns]
        out_ref[head, :deep, HEAD:] = picks
        out_ref[head, deep:, HEAD:] = jnp.zeros_like(picks)


def project_latents(source, own, swapped):
    chips, here = lax.axis_size("chip"), lax.axis_index("chip")
    step = jnp.where(lax.axis_index("core") == 0, 1, -1)
    rows, columns = own[0].shape
    counts = [batch.shape[0] // rows for batch in swapped]
    hops = list(range(len(own))) + [-hop for hop in range(1, sum(counts) + 1)]
    places = lax.rem(here - jnp.array(hops, jnp.int32) * step + chips, chips)
    whole = pl.BlockSpec(memory_space=pltpu.VMEM)
    return pl.pallas_call(
        functools.partial(project_body, counts),
        in_specs=[pl.BlockSpec(memory_space=pltpu.SMEM)] + [whole] * (1 + len(own) + len(swapped)),
        out_specs=whole,
        out_shape=jax.ShapeDtypeStruct((columns // HEAD, source.shape[0], 2 * HEAD), jnp.bfloat16),
        scratch_shapes=[pltpu.VMEM((chips * rows, columns), jnp.bfloat16)],
        cost_estimate=pl.CostEstimate(
            flops=2 * source.size * columns,
            bytes_accessed=2 * source.size + 4 * chips * rows * columns,
            transcendentals=0,
        ),
        name="project",
    )(places, source, *own, *swapped)


def time_embed(sigma_now, half_count):
    frequency = jnp.exp(
        -math.log(10000.0) * jnp.arange(half_count).astype(jnp.float32) / half_count
    )
    angles = 1000.0 * sigma_now * frequency
    return jnp.concatenate([jnp.cos(angles), jnp.sin(angles)])


def pack_body(key_ref, value_ref, latent_ref, spread_ref, out_ref):
    rows = key_ref.shape[0]
    channels, tokens = latent_ref.shape
    out_ref[0, :rows] = key_ref[...]
    out_ref[0, rows : 2 * rows] = value_ref[...]
    spread = spread_ref[...]
    coarse = spread.astype(jnp.bfloat16).astype(jnp.float32)
    tail = jnp.concatenate(
        [
            latent_ref[...],
            jnp.ones_like(spread),
            coarse,
            spread - coarse,
            jnp.zeros((EXTRA - 3, tokens), jnp.float32),
        ]
    )
    out_ref[0, 2 * rows :] = jnp.zeros((channels + EXTRA, out_ref.shape[2]), jnp.bfloat16)
    out_ref[0, 2 * rows :, :tokens] = tail.astype(jnp.bfloat16)


def pack(keys, values, latent, spread, parts):
    rows, width = keys.shape
    channels, tokens = latent.shape
    columns = width // parts
    height = 2 * rows + channels + EXTRA
    return pl.pallas_call(
        pack_body,
        grid=(parts,),
        in_specs=[
            pl.BlockSpec((rows, columns), lambda p: (0, p)),
            pl.BlockSpec((rows, columns), lambda p: (0, p)),
            pl.BlockSpec((channels, tokens), lambda p: (0, 0)),
            pl.BlockSpec((1, tokens), lambda p: (0, 0)),
        ],
        out_specs=pl.BlockSpec((1, height, columns), lambda p: (p, 0, 0)),
        out_shape=jax.ShapeDtypeStruct((parts, height, columns), jnp.bfloat16),
        cost_estimate=pl.CostEstimate(
            flops=parts * height * columns,
            bytes_accessed=4 * parts * height * columns,
            transcendentals=0,
        ),
        name="pack",
    )(keys, values, latent, spread)


def attention_body(parts, rows, tile, packed_ref, project_ref, gain_ref, out_ref):
    columns = pl.ds(pl.multiple_of(pl.program_id(0) * HEAD, HEAD), HEAD)
    keys = packed_ref[:, :rows, columns].reshape(-1, HEAD)
    values = packed_ref[:, rows : 2 * rows, columns].reshape(-1, HEAD)
    queries = []
    for part in range(parts):
        tokens = packed_ref[part, 2 * rows :, :tile]
        both = lax.dot_general(
            jnp.concatenate([tokens, tokens]),
            project_ref[0],
            (((0,), (0,)), ((), ())),
            preferred_element_type=jnp.float32,
        )
        raw, spread = both[:, :HEAD], both[:, HEAD:]
        square = jnp.mean(raw * raw, axis=-1, keepdims=True) + epsilon * (spread * spread)
        queries.append((raw * lax.rsqrt(square) * gain_ref[...]).astype(jnp.bfloat16))
    scores = [
        lax.dot_general(q, keys, (((1,), (1,)), ((), ())), preferred_element_type=jnp.float32)
        for q in queries
    ]
    for part in range(parts):
        peak = jnp.max(scores[part], axis=-1, keepdims=True)
        weights = jnp.exp((scores[part] - peak) * (1.0 / math.sqrt(HEAD)))
        total = jnp.sum(weights, axis=-1, keepdims=True)
        blended = jnp.dot(weights.astype(jnp.bfloat16), values, preferred_element_type=jnp.float32)
        out_ref[part] = (blended / total).astype(jnp.bfloat16)


def attention(project, query_gain, packed, rows, tile):
    parts, height, width = packed.shape
    tokens = parts * tile
    heads = width // HEAD
    work = tokens * parts * rows * width
    whole = pl.BlockSpec(memory_space=pltpu.VMEM)
    return pl.pallas_call(
        functools.partial(attention_body, parts, rows, tile),
        grid=(heads,),
        in_specs=[whole, pl.BlockSpec((1, *project.shape[1:]), lambda h: (h, 0, 0)), whole],
        out_specs=pl.BlockSpec((parts, tile, HEAD), lambda h: (0, 0, h)),
        out_shape=jax.ShapeDtypeStruct((parts, tile, width), jnp.bfloat16),
        cost_estimate=pl.CostEstimate(
            flops=4 * work,
            bytes_accessed=4 * parts * rows * width + 6 * tokens * width,
            transcendentals=work // HEAD,
        ),
        name="attention",
    )(packed, project, query_gain.reshape(1, HEAD))


def prefix_over_steps(drift):
    half = jnp.bfloat16

    def wide(value):
        return value.astype(jnp.float32)

    other = wide(swap_cores(drift.astype(half)))
    within = jnp.where(lax.axis_index("core") == 1, other, jnp.zeros_like(other))
    here = drift + other
    near = wide(shift(here.astype(half), "chip", 1, False))
    near = near + wide(shift((here + near).astype(half), "chip", 2, False))
    window = (here + near).astype(half)
    chips = lax.axis_size("chip")
    far = send_by_core(window, 4, chips - 4, False)
    far = wide(far) + wide(send_by_core(far, 4, None, False))
    return within + near + far + wide(swap_cores(far.astype(half)))


def per_device(
    latent_old,
    noise_start,
    step_index,
    sigma_table,
    mod_weight,
    embed_weight,
    embed_bias,
    query_weight,
    query_gain,
    stale_keys,
    stale_values,
    out_weight,
    final_weight,
):
    parts, part = lax.axis_size("patch"), lax.axis_index("patch")
    width = embed_weight.shape[1]
    columns = query_weight.shape[1] // parts
    latent = latent_old[0].T
    channels, token_count = latent.shape
    key_rows = stale_keys.shape[1]

    core = lax.axis_index("core")


    def embed(latent, embed_weight, embed_bias):
        hidden = lax.dot_general(
            latent.astype(jnp.bfloat16),
            embed_weight,
            (((0,), (0,)), ((), ())),
            preferred_element_type=jnp.float32,
        )
        hidden = hidden + embed_bias
        row_mean = jnp.mean(hidden, axis=-1, keepdims=True)
        row_var = jnp.mean(jnp.square(hidden - row_mean), axis=-1)
        return hidden, jnp.sqrt(row_var + epsilon)[None]

    def modulation(step_index, sigma_table, mod_weight):
        slots = jnp.arange(sigma_table.shape[0])
        sigma_now = jnp.sum(jnp.where(slots == step_index[0], sigma_table, 0.0))
        sigma_next = jnp.sum(jnp.where(slots == step_index[0] + 1, sigma_table, 0.0))
        embedded = jax.nn.silu(time_embed(sigma_now, mod_weight.shape[0] // 2)).astype(jnp.bfloat16)
        modulate = jnp.dot(embedded[None, :], mod_weight, preferred_element_type=jnp.float32)[0]
        return modulate, sigma_next - sigma_now

    def split(value):
        coarse = value.astype(jnp.bfloat16)
        return jnp.concatenate([coarse, (value - coarse.astype(jnp.float32)).astype(jnp.bfloat16)])

    def sources(modulate, embed_weight, embed_bias):
        shift_vec, scale_vec = modulate[:width], modulate[width : 2 * width]
        weight = embed_weight.astype(jnp.float32)
        centered = jnp.concatenate(
            [
                weight - jnp.mean(weight, axis=-1, keepdims=True),
                (embed_bias - jnp.mean(embed_bias))[None],
            ]
        )
        rows = [
            centered * (1.0 + scale_vec),
            shift_vec[None],
            shift_vec[None],
            jnp.zeros((EXTRA - 3, width), jnp.float32),
        ]
        return split(jnp.concatenate(rows))

    my_columns = lax.dynamic_slice_in_dim(query_weight, part * columns, columns, 1)
    tasks = {
        1: (embed, (latent, embed_weight, embed_bias)),
        2: (
            functools.partial(pack, parts=parts),
            lambda done: (stale_keys[0], stale_values[0], latent, done[1][1]),
        ),
        4: (modulation, (step_index, sigma_table, mod_weight)),
        6: (sources, lambda done: (done[4][0], embed_weight, embed_bias)),
    }
    other = swap_cores(my_columns)
    piece = [jnp.where(core == 0, my_columns, other), jnp.where(core == 0, other, my_columns)]
    own, swapped, done = pass_round(jnp.concatenate(piece), tasks)
    hidden, (modulate, delta), source = done[1][0], done[4], done[6]
    _, late = lax.optimization_barrier((own[GATHER_AFTER], out_weight))
    all_out_weight = lax.all_gather(late, STEP, axis=0, tiled=True)
    packed = lax.all_to_all(done[2], "patch", 0, 0, tiled=True)

    project = project_latents(source, own, swapped)
    attended = attention(project, query_gain, packed, key_rows, token_count)
    attended = lax.all_to_all(attended, "patch", 0, 0, tiled=True)
    attended = jnp.moveaxis(attended, 0, 1).reshape(token_count, -1)
    branch = lax.dot_general(
        attended, all_out_weight, (((1,), (1,)), ((), ())), preferred_element_type=jnp.float32
    )
    mixed = hidden + modulate[2 * width :] * branch
    centered = mixed - jnp.mean(mixed, axis=-1, keepdims=True)
    variance = jnp.mean(jnp.square(centered), axis=-1, keepdims=True)
    normed = (centered * lax.rsqrt(variance + epsilon)).astype(jnp.bfloat16)
    velocity = lax.dot_general(
        final_weight, normed, (((0,), (1,)), ((), ())), preferred_element_type=jnp.float32
    )
    drift = velocity * delta
    return (noise_start.T + (prefix_over_steps(drift) + drift)).T[None]


def solution(mesh):
    shape = mesh.shape
    torus = Mesh(
        mesh.devices.reshape(shape["rep"], shape["step"] // CORES, CORES, shape["patch"]),
        ("rep", "chip", "core", "patch"),
    )
    placed = (
        P(REP_STEP, "patch", None),
        P(("rep", "patch"), None),
        P(REP_STEP),
        P(),
        P(),
        P(),
        P(),
        P(STEP, None),
        P(),
        P(REP_STEP, "patch", None),
        P(REP_STEP, "patch", None),
        P(STEP, None),
        P(),
    )
    return jax.shard_map(
        per_device,
        mesh=torus,
        in_specs=placed,
        out_specs=P(REP_STEP, "patch", None),
        check_vma=False,
    )
```

```python
import functools
import math

import jax
import jax.numpy as jnp
from jax import lax
from jax.experimental import pallas as pl
from jax.experimental.pallas import tpu as pltpu
from jax.sharding import Mesh
from jax.sharding import PartitionSpec as P

HEAD = 128
CORES = 2
EXTRA = 16
GATHER_AFTER = 3
STEP = ("chip", "core")
REP_STEP = ("rep", "chip", "core")
epsilon = 1e-06


def shift(value, axis, distance, wrap):
    size = lax.axis_size(axis)
    pairs = [(i, (i + distance) % size) for i in range(size) if wrap or 0 <= i + distance < size]
    return lax.ppermute(value, axis, pairs)


def swap_cores(value):
    return lax.ppermute(value, "core", [(0, 1), (1, 0)])


def send_by_core(value, first, second, wrap):
    chips = lax.axis_size("chip")
    pairs = []
    for core, distance in enumerate((first, second)):
        for chip in range(chips):
            target = chip + (distance or 0)
            if distance is not None and (wrap or 0 <= target < chips):
                pairs.append((chip * CORES + core, target % chips * CORES + core))
    return lax.ppermute(value, ("chip", "core"), pairs)


def pass_round(piece, tasks):
    half = lax.axis_size("chip") // 2
    own, swapped, waiting, results = [piece], [], [], {}
    for hop in range(1, half + 1):
        sent = send_by_core(piece, 1, -1, True)
        if hop in tasks:
            task, inputs = tasks[hop]
            if callable(inputs):
                inputs = inputs(results)
            _, inputs = lax.optimization_barrier((piece, inputs))
            results[hop] = task(*inputs)
            sent, results[hop] = lax.optimization_barrier((sent, results[hop]))
        piece = sent
        own.append(piece)
        waiting.append(piece)
        if hop in (half // 2, half - 1):
            swapped.append(swap_cores(jnp.concatenate(waiting)))
            waiting = []
    return own, swapped, results


def project_body(counts, place_ref, source_ref, *refs):
    own, swapped, out_ref, joined_ref = refs[:-4], refs[-4:-2], refs[-2], refs[-1]
    rows = own[0].shape[0]

    def put(value, slot):
        joined_ref[pl.ds(pl.multiple_of(place_ref[slot] * rows, rows), rows)] = value

    for hop, piece in enumerate(own):
        put(piece[...], hop)
    slot = len(own)
    for count, batch in zip(counts, swapped):
        for i in range(count):
            put(batch[i * rows : (i + 1) * rows], slot)
            slot += 1
    total = jnp.dot(source_ref[...], joined_ref[...], preferred_element_type=jnp.float32)
    deep = total.shape[0] // 2
    total = total[:deep] + total[deep:]
    coarse = total.astype(jnp.bfloat16)
    fine = (total - coarse.astype(jnp.float32)).astype(jnp.bfloat16)
    row = lax.broadcasted_iota(jnp.int32, (deep, HEAD), 0)
    spread = (row == deep - EXTRA + 1) | (row == deep - EXTRA + 2)
    picks = jnp.where(spread, 1.0, 0.0).astype(jnp.bfloat16)
    for head in range(out_ref.shape[0]):
        columns = slice(head * HEAD, (head + 1) * HEAD)
        out_ref[head, :deep, :HEAD] = coarse[:, columns]
        out_ref[head, deep:, :HEAD] = fine[:, columns]
        out_ref[head, :deep, HEAD:] = picks
        out_ref[head, deep:, HEAD:] = jnp.zeros_like(picks)


def project_latents(source, own, swapped):
    chips, here = lax.axis_size("chip"), lax.axis_index("chip")
    step = jnp.where(lax.axis_index("core") == 0, 1, -1)
    rows, columns = own[0].shape
    counts = [batch.shape[0] // rows for batch in swapped]
    hops = list(range(len(own))) + [-hop for hop in range(1, sum(counts) + 1)]
    places = lax.rem(here - jnp.array(hops, jnp.int32) * step + chips, chips)
    whole = pl.BlockSpec(memory_space=pltpu.VMEM)
    return pl.pallas_call(
        functools.partial(project_body, counts),
        in_specs=[pl.BlockSpec(memory_space=pltpu.SMEM)] + [whole] * (1 + len(own) + len(swapped)),
        out_specs=whole,
        out_shape=jax.ShapeDtypeStruct((columns // HEAD, source.shape[0], 2 * HEAD), jnp.bfloat16),
        scratch_shapes=[pltpu.VMEM((chips * rows, columns), jnp.bfloat16)],
        cost_estimate=pl.CostEstimate(
            flops=2 * source.size * columns,
            bytes_accessed=2 * source.size + 4 * chips * rows * columns,
            transcendentals=0,
        ),
        name="project",
    )(places, source, *own, *swapped)


def time_embed(sigma_now, half_count):
    frequency = jnp.exp(
        -math.log(10000.0) * jnp.arange(half_count).astype(jnp.float32) / half_count
    )
    angles = 1000.0 * sigma_now * frequency
    return jnp.concatenate([jnp.cos(angles), jnp.sin(angles)])


def pack_body(key_ref, value_ref, latent_ref, spread_ref, out_ref):
    rows = key_ref.shape[0]
    channels, tokens = latent_ref.shape
    out_ref[0, :rows] = key_ref[...]
    out_ref[0, rows : 2 * rows] = value_ref[...]
    spread = spread_ref[...]
    coarse = spread.astype(jnp.bfloat16).astype(jnp.float32)
    tail = jnp.concatenate(
        [
            latent_ref[...],
            jnp.ones_like(spread),
            coarse,
            spread - coarse,
            jnp.zeros((EXTRA - 3, tokens), jnp.float32),
        ]
    )
    out_ref[0, 2 * rows :] = jnp.zeros((channels + EXTRA, out_ref.shape[2]), jnp.bfloat16)
    out_ref[0, 2 * rows :, :tokens] = tail.astype(jnp.bfloat16)


def pack(keys, values, latent, spread, parts):
    rows, width = keys.shape
    channels, tokens = latent.shape
    columns = width // parts
    height = 2 * rows + channels + EXTRA
    return pl.pallas_call(
        pack_body,
        grid=(parts,),
        in_specs=[
            pl.BlockSpec((rows, columns), lambda p: (0, p)),
            pl.BlockSpec((rows, columns), lambda p: (0, p)),
            pl.BlockSpec((channels, tokens), lambda p: (0, 0)),
            pl.BlockSpec((1, tokens), lambda p: (0, 0)),
        ],
        out_specs=pl.BlockSpec((1, height, columns), lambda p: (p, 0, 0)),
        out_shape=jax.ShapeDtypeStruct((parts, height, columns), jnp.bfloat16),
        cost_estimate=pl.CostEstimate(
            flops=parts * height * columns,
            bytes_accessed=4 * parts * height * columns,
            transcendentals=0,
        ),
        name="pack",
    )(keys, values, latent, spread)


def attention_body(parts, rows, tile, packed_ref, project_ref, gain_ref, out_ref):
    columns = pl.ds(pl.multiple_of(pl.program_id(0) * HEAD, HEAD), HEAD)
    keys = packed_ref[:, :rows, columns].reshape(-1, HEAD)
    values = packed_ref[:, rows : 2 * rows, columns].reshape(-1, HEAD)
    queries = []
    for part in range(parts):
        tokens = packed_ref[part, 2 * rows :, :tile]
        both = lax.dot_general(
            jnp.concatenate([tokens, tokens]),
            project_ref[0],
            (((0,), (0,)), ((), ())),
            preferred_element_type=jnp.float32,
        )
        raw, spread = both[:, :HEAD], both[:, HEAD:]
        square = jnp.mean(raw * raw, axis=-1, keepdims=True) + epsilon * (spread * spread)
        queries.append((raw * lax.rsqrt(square) * gain_ref[...]).astype(jnp.bfloat16))
    scores = [
        lax.dot_general(q, keys, (((1,), (1,)), ((), ())), preferred_element_type=jnp.float32)
        for q in queries
    ]
    for part in range(parts):
        peak = jnp.max(scores[part], axis=-1, keepdims=True)
        weights = jnp.exp((scores[part] - peak) * (1.0 / math.sqrt(HEAD)))
        total = jnp.sum(weights, axis=-1, keepdims=True)
        blended = jnp.dot(weights.astype(jnp.bfloat16), values, preferred_element_type=jnp.float32)
        out_ref[part] = (blended / total).astype(jnp.bfloat16)


def attention(project, query_gain, packed, rows, tile):
    parts, height, width = packed.shape
    tokens = parts * tile
    heads = width // HEAD
    work = tokens * parts * rows * width
    whole = pl.BlockSpec(memory_space=pltpu.VMEM)
    return pl.pallas_call(
        functools.partial(attention_body, parts, rows, tile),
        grid=(heads,),
        in_specs=[whole, pl.BlockSpec((1, *project.shape[1:]), lambda h: (h, 0, 0)), whole],
        out_specs=pl.BlockSpec((parts, tile, HEAD), lambda h: (0, 0, h)),
        out_shape=jax.ShapeDtypeStruct((parts, tile, width), jnp.bfloat16),
        cost_estimate=pl.CostEstimate(
            flops=4 * work,
            bytes_accessed=4 * parts * rows * width + 6 * tokens * width,
            transcendentals=work // HEAD,
        ),
        name="attention",
    )(packed, project, query_gain.reshape(1, HEAD))


def prefix_over_steps(drift):
    half = jnp.bfloat16

    def wide(value):
        return value.astype(jnp.float32)

    other = wide(swap_cores(drift.astype(half)))
    within = jnp.where(lax.axis_index("core") == 1, other, jnp.zeros_like(other))
    here = drift + other
    near = wide(shift(here.astype(half), "chip", 1, False))
    near = near + wide(shift((here + near).astype(half), "chip", 2, False))
    window = (here + near).astype(half)
    chips = lax.axis_size("chip")
    far = send_by_core(window, 4, chips - 4, False)
    far = wide(far) + wide(send_by_core(far, 4, None, False))
    return within + near + far + wide(swap_cores(far.astype(half)))


def per_device(
    latent_old,
    noise_start,
    step_index,
    sigma_table,
    mod_weight,
    embed_weight,
    embed_bias,
    query_weight,
    query_gain,
    stale_keys,
    stale_values,
    out_weight,
    final_weight,
):
    parts, part = lax.axis_size("patch"), lax.axis_index("patch")
    width = embed_weight.shape[1]
    columns = query_weight.shape[1] // parts
    latent = latent_old[0].T
    channels, token_count = latent.shape
    key_rows = stale_keys.shape[1]

    core = lax.axis_index("core")


    def embed(latent, embed_weight, embed_bias):
        hidden = lax.dot_general(
            latent.astype(jnp.bfloat16),
            embed_weight,
            (((0,), (0,)), ((), ())),
            preferred_element_type=jnp.float32,
        )
        hidden = hidden + embed_bias
        row_mean = jnp.mean(hidden, axis=-1, keepdims=True)
        row_var = jnp.mean(jnp.square(hidden - row_mean), axis=-1)
        return hidden, jnp.sqrt(row_var + epsilon)[None]

    def modulation(step_index, sigma_table, mod_weight):
        slots = jnp.arange(sigma_table.shape[0])
        sigma_now = jnp.sum(jnp.where(slots == step_index[0], sigma_table, 0.0))
        sigma_next = jnp.sum(jnp.where(slots == step_index[0] + 1, sigma_table, 0.0))
        embedded = jax.nn.silu(time_embed(sigma_now, mod_weight.shape[0] // 2)).astype(jnp.bfloat16)
        modulate = jnp.dot(embedded[None, :], mod_weight, preferred_element_type=jnp.float32)[0]
        return modulate, sigma_next - sigma_now

    def split(value):
        coarse = value.astype(jnp.bfloat16)
        return jnp.concatenate([coarse, (value - coarse.astype(jnp.float32)).astype(jnp.bfloat16)])

    def sources(modulate, embed_weight, embed_bias):
        shift_vec, scale_vec = modulate[:width], modulate[width : 2 * width]
        weight = embed_weight.astype(jnp.float32)
        centered = jnp.concatenate(
            [
                weight - jnp.mean(weight, axis=-1, keepdims=True),
                (embed_bias - jnp.mean(embed_bias))[None],
            ]
        )
        rows = [
            centered * (1.0 + scale_vec),
            shift_vec[None],
            shift_vec[None],
            jnp.zeros((EXTRA - 3, width), jnp.float32),
        ]
        return split(jnp.concatenate(rows))

    my_columns = lax.dynamic_slice_in_dim(query_weight, part * columns, columns, 1)
    tasks = {
        1: (embed, (latent, embed_weight, embed_bias)),
        2: (
            functools.partial(pack, parts=parts),
            lambda done: (stale_keys[0], stale_values[0], latent, done[1][1]),
        ),
        4: (modulation, (step_index, sigma_table, mod_weight)),
        6: (sources, lambda done: (done[4][0], embed_weight, embed_bias)),
    }
    other = swap_cores(my_columns)
    piece = [jnp.where(core == 0, my_columns, other), jnp.where(core == 0, other, my_columns)]
    own, swapped, done = pass_round(jnp.concatenate(piece), tasks)
    hidden, (modulate, delta), source = done[1][0], done[4], done[6]
    _, late = lax.optimization_barrier((own[GATHER_AFTER], out_weight))
    all_out_weight = lax.all_gather(late, STEP, axis=0, tiled=True)
    packed = lax.all_to_all(done[2], "patch", 0, 0, tiled=True)

    project = project_latents(source, own, swapped)
    attended = attention(project, query_gain, packed, key_rows, token_count)
    attended = lax.all_to_all(attended, "patch", 0, 0, tiled=True)
    attended = jnp.moveaxis(attended, 0, 1).reshape(token_count, -1)
    branch = lax.dot_general(
        attended, all_out_weight, (((1,), (1,)), ((), ())), preferred_element_type=jnp.float32
    )
    mixed = hidden + modulate[2 * width :] * branch
    centered = mixed - jnp.mean(mixed, axis=-1, keepdims=True)
    variance = jnp.mean(jnp.square(centered), axis=-1, keepdims=True)
    normed = (centered * lax.rsqrt(variance + epsilon)).astype(jnp.bfloat16)
    velocity = lax.dot_general(
        final_weight, normed, (((0,), (1,)), ((), ())), preferred_element_type=jnp.float32
    )
    drift = velocity * delta
    return (noise_start.T + (prefix_over_steps(drift) + drift)).T[None]


def solution(mesh):
    shape = mesh.shape
    torus = Mesh(
        mesh.devices.reshape(shape["rep"], shape["step"] // CORES, CORES, shape["patch"]),
        ("rep", "chip", "core", "patch"),
    )
    placed = (
        P(REP_STEP, "patch", None),
        P(("rep", "patch"), None),
        P(REP_STEP),
        P(),
        P(),
        P(),
        P(),
        P(STEP, None),
        P(),
        P(REP_STEP, "patch", None),
        P(REP_STEP, "patch", None),
        P(STEP, None),
        P(),
    )
    return jax.shard_map(
        per_device,
        mesh=torus,
        in_specs=placed,
        out_specs=P(REP_STEP, "patch", None),
        check_vma=False,
    )
```
